128 devices in a mesh: band: 32 (over y, x, core), lev: 4 (over z).
Axes of the slice: x: 4, y: 4, z: 4, core: 2. Of those that a mesh axis runs over, the one named last changes fastest.
Arguments:
- field_grid: float32 [3, 16, 384, 2, 1536], P(None, 'lev', 'band'), may hold values from -6 to 6
- increment: float32 [3, 16, 384, 2, 1536], P(None, 'lev', 'band'), may hold values from -6 to 6
- points: int32 [384], P('band'), may hold values from 16 to 1536, as said below
- weights: float32 [384], replicated, may hold values from 0.0013020834 to 0.0052083335
- pair_slot: int32 [384], replicated, may hold values from 0 to 383, each once
- legendre: float32 [384, 384, 769], P(('band', 'lev')), may hold values from -6 to 6
- strength: float32 [3, 16], replicated, may hold values from 1 to 16
Outputs:
- stepped: float32 [3, 16, 384, 2, 1536], P(None, 'lev', 'band')
The draws below stay inside these ranges and needn't reach their ends.
Inputs may be any that keep to these rules, and one draw needn't show every extreme that they name: points[j] lies within 32 of 16 + 1520 * j // 383, kept within 16 to 1536; the last latitude pair has 1536 cells. `pair_slot`: A permutation of 0 to 383; slot s is held by the device of joint band+lev index s // 3, at place s % 3, which holds legendre[s].
All inputs are finite; a program needn't handle non-finite values.
Results may differ from the reference program's by a relative error of at most 0.0003.
Values sent between devices are 32-bit elements; how exact they have to be, the bound alone decides.
A program may use at most 128 MiB of HBM per device.

```python
import math
import jax
import jax.numpy as jnp
from jax import lax

WAVES = 768
FIELDS = 3
HALF = 384
NLON = 1536
LEVELS = 16


def draw_points(key, part):
    pair_index = lax.iota(jnp.int32, HALF)
    smooth_count = 16 + (2 * WAVES - 16) * pair_index // (HALF - 1)
    jitter = jax.random.randint(key, (HALF,), -32, 33)
    counts = jnp.clip(smooth_count + jitter, 16, 2 * WAVES)
    return jnp.where(pair_index == HALF - 1, 2 * WAVES, counts).astype(jnp.int32)


def levels(own_key, dims, cuts, least, high):
    level, own = 1.0, jax.random.fold_in(own_key, 6)
    for position, shards_of in cuts:
        draws = jnp.exp(jax.random.uniform(jax.random.fold_in(own, position), (shards_of,), jnp.float32, least / len(cuts), high / len(cuts)))
        level = level * jnp.repeat(draws, dims[position] // shards_of).reshape([-1 if axis == position else 1 for axis in range(len(dims))])
    return level


def normal_values(rng, shape, spread, bound, cuts=(), kind=jnp.bfloat16):
    entries = jax.random.normal(rng, shape, jnp.float32) * spread
    if len(cuts) > 0:
        entries = levels(rng, shape, cuts, -0.22, 0.18) * entries
    return jnp.clip(entries, min=-bound, max=bound).astype(kind)


def setup_inputs(seed: int = 0) -> dict:
    arg_keys = jax.random.split(jax.random.key(seed), 8)
    return {
        "field_grid": normal_values(arg_keys[0], (FIELDS, LEVELS, HALF, 2, NLON), 1.0, 6.0, ((1, 4), (2, 32)), jnp.float32),
        "increment": normal_values(arg_keys[1], (FIELDS, LEVELS, HALF, 2, NLON), 1.0, 6.0, ((1, 4), (2, 32)), jnp.float32),
        "points": draw_points(jax.random.fold_in(arg_keys[7], 71), 0),
        "weights": jnp.clip(jnp.exp(jax.random.uniform(arg_keys[3], (HALF,), jnp.float32, math.log(0.0013020834), math.log(0.0052083335))), 0.0013020834, 0.0052083335),
        "pair_slot": jax.random.permutation(arg_keys[4], HALF).astype(jnp.int32),
        "legendre": normal_values(arg_keys[5], (HALF, HALF, WAVES + 1), 1.0, 6.0, ((0, 128),), jnp.float32),
        "strength": jnp.clip(jnp.exp(jax.random.uniform(arg_keys[6], (FIELDS, LEVELS), jnp.float32, math.log(1.0), math.log(16.0))), 1.0, 16.0),
    }


TWO_PI = 2.0 * math.pi


def dft_basis(count):
    places = lax.iota(jnp.int32, NLON)
    orders = lax.iota(jnp.int32, WAVES)
    turns = (places[:, None] * orders[None, :]) % count
    angle = turns.astype(jnp.float32) * (TWO_PI / count.astype(jnp.float32))
    live = (places[:, None] < count) & (orders[None, :] <= (count - 1) // 2)
    cosines = jnp.where(live, jnp.cos(angle), 0.0)
    sines = jnp.where(live, -jnp.sin(angle), 0.0)
    return jnp.concatenate([cosines, sines], axis=1)


def reference(field_grid, increment, points, weights, pair_slot, legendre, strength):
    summed = field_grid + increment
    row_count = FIELDS * LEVELS * 2
    by_pair = jnp.moveaxis(summed, 2, 0).reshape(HALF, row_count, NLON)

    def forward(item):
        block, count = item
        product = jnp.dot(block, dft_basis(count), precision=lax.Precision.HIGHEST)
        return product / count.astype(jnp.float32)

    spectra = lax.map(forward, (by_pair, points))
    spectra = spectra.reshape(HALF, FIELDS * LEVELS, 2, 2, WAVES)
    columns = lax.iota(jnp.int32, WAVES + 1)
    degree_top = float((WAVES - 1) * WAVES)
    damping_rate = strength.reshape(FIELDS * LEVELS)

    def per_pair(lower_wave):
        table = lax.dynamic_index_in_dim(legendre, pair_slot[lower_wave], 0, keepdims=False)
        higher_wave = WAVES - 1 - lower_wave
        first = lax.dynamic_index_in_dim(spectra, lower_wave, 4, keepdims=False)
        second = lax.dynamic_index_in_dim(spectra, higher_wave, 4, keepdims=False)
        second_member = columns >= WAVES - lower_wave
        degree = jnp.where(second_member, columns - 1, lower_wave + columns)
        wave_of_column = jnp.where(second_member, higher_wave, lower_wave)
        parity = jnp.where((degree - wave_of_column) % 2 == 0, 1.0, -1.0)
        first_weighted = (first * weights[:, None, None, None]).reshape(HALF, -1)
        second_weighted = (second * weights[:, None, None, None]).reshape(HALF, -1)
        part_first = jnp.dot(table.T, first_weighted, precision=lax.Precision.HIGHEST)
        part_second = jnp.dot(table.T, second_weighted, precision=lax.Precision.HIGHEST)
        part_first = part_first.reshape(WAVES + 1, FIELDS * LEVELS, 2, 2)
        part_second = part_second.reshape(WAVES + 1, FIELDS * LEVELS, 2, 2)
        chosen = jnp.where(second_member[:, None, None, None], part_second, part_first)
        coefficients = chosen[:, :, 0, :] + parity[:, None, None] * chosen[:, :, 1, :]
        degree_real = degree.astype(jnp.float32)
        degree_ratio = degree_real * (degree_real + 1.0) / degree_top
        damping = 1.0 / (1.0 + damping_rate[None, :] * (degree_ratio * degree_ratio)[:, None])
        damped = coefficients * damping[:, :, None]
        lower_part = jnp.where(second_member[:, None, None], 0.0, damped)
        upper_part = jnp.where(second_member[:, None, None], damped, 0.0)
        stacked = jnp.stack([lower_part, lower_part * parity[:, None, None],
                             upper_part, upper_part * parity[:, None, None]], axis=1)
        returned = jnp.dot(table, stacked.reshape(WAVES + 1, -1), precision=lax.Precision.HIGHEST)
        returned = returned.reshape(HALF, 2, 2, FIELDS * LEVELS, 2)
        return returned[:, 0], returned[:, 1]

    first_back, second_back = lax.map(per_pair, lax.iota(jnp.int32, HALF))
    by_wave = jnp.concatenate([first_back, second_back[::-1]], axis=0)
    spectral_rows = jnp.transpose(by_wave, (1, 3, 2, 4, 0)).reshape(HALF, row_count, 2 * WAVES)
    doubling = jnp.where(lax.iota(jnp.int32, 2 * WAVES) % WAVES == 0, 1.0, 2.0)

    def inverse(item):
        block, count = item
        return jnp.dot(block * doubling[None, :], dft_basis(count).T, precision=lax.Precision.HIGHEST)

    grid_rows = lax.map(inverse, (spectral_rows, points))
    grid_rows = grid_rows.reshape(HALF, FIELDS, LEVELS, 2, NLON)
    return jnp.moveaxis(grid_rows, 0, 2)
```

```python
import functools
import math

import jax
import jax.numpy as jnp
from jax import lax
from jax.experimental import pallas as pl
from jax.experimental.pallas import tpu as pltpu
from jax.sharding import PartitionSpec as P

MESH = pl.DeviceIdType.MESH
F32 = jnp.float32
BF16 = jnp.bfloat16
SIN_COEFS = [(-1) ** k * math.pi ** (2 * k + 1) / math.factorial(2 * k + 1) for k in range(7)]
COS_COEFS = [(-1) ** k * math.pi ** (2 * k) / math.factorial(2 * k) for k in range(8)]


def half_turn_pair(half):
    square = half * half
    sine = jnp.full_like(square, SIN_COEFS[-1])
    for coef in SIN_COEFS[-2::-1]:
        sine = sine * square + coef
    cosine = jnp.full_like(square, COS_COEFS[-1])
    for coef in COS_COEFS[-2::-1]:
        cosine = cosine * square + coef
    return cosine, sine * half


def turn_pair(orders, doubled, count):
    period = 2.0 * count
    product = orders * doubled
    rest = product - jnp.round(product / period) * period
    cosine, sine = half_turn_pair(rest / period)
    return 1.0 - 2.0 * sine * sine, 2.0 * sine * cosine


def split(value):
    high = value.astype(BF16)
    return high, (value - high.astype(F32)).astype(BF16)


def wide_dot(left, right, contract):
    return lax.dot_general(left, right, (contract, ((), ())), preferred_element_type=F32)


def phase_rows(orders, count):
    row = lax.broadcasted_iota(jnp.int32, (8, orders.shape[1]), 0)
    fine = 2 * row + 1
    step = jnp.where(row < 4, jnp.left_shift(16, jnp.minimum(row, 4)), (row - 4) * 512 + 256)
    step = jnp.where(row == 7, 1535, step)
    wide = jnp.broadcast_to(orders, (8, orders.shape[1]))
    fine_pair = turn_pair(wide, fine.astype(F32), count)
    step_pair = turn_pair(wide, step.astype(F32), count)
    return fine_pair, step_pair


def fill_tables(fine_pair, step_pair, cos_hi, cos_lo, sin_hi, sin_lo):
    cosine, sine = fine_pair
    step_cos, step_sin = step_pair
    for level in range(4):
        turn_cos = step_cos[level : level + 1]
        turn_sin = step_sin[level : level + 1]
        next_cos = cosine * turn_cos - sine * turn_sin
        next_sin = sine * turn_cos + cosine * turn_sin
        cosine = jnp.concatenate([cosine, next_cos], axis=0)
        sine = jnp.concatenate([sine, next_sin], axis=0)
    high, low = split(cosine)
    cos_hi[...] = high
    cos_lo[...] = low
    high, low = split(sine)
    sin_hi[...] = high
    sin_lo[...] = low


def reversed_lanes(value):
    index = 127 - lax.broadcasted_iota(jnp.int32, value.shape, 1)
    return jnp.take_along_axis(value, index, axis=1)


def forward_kernel(points, weights, orders_ref, field, increment, out, rows, spectra, cos_hi, cos_lo, sin_hi, sin_lo):
    pair = pl.program_id(0)
    for f in range(3):
        for l in range(4):
            at = 8 * f + 2 * l
            rows[at : at + 2, :] = field[f, l, 0] + increment[f, l, 0]
    count = points[0, pair].astype(F32)
    band = lax.axis_index("band")
    weight = weights[band * 12 + pair]
    orders = orders_ref[...]
    fine_pair, step_pair = phase_rows(orders, count)
    fill_tables(fine_pair, step_pair, cos_hi, cos_lo, sin_hi, sin_lo)
    step_cos, step_sin = step_pair
    value = rows[...]
    place = lax.broadcasted_iota(jnp.int32, value.shape, 1).astype(F32)
    value = jnp.where(place < count, value, 0.0)
    even, odd = [], []
    for block in range(6):
        low = reversed_lanes(value[:, 256 * block : 256 * block + 128])
        high = value[:, 256 * block + 128 : 256 * block + 256]
        even.append(high + low)
        odd.append(high - low)

    def folded(parts):
        return jnp.concatenate(
            [parts[3 + g] + parts[2 - g] for g in range(3)] + [parts[3 + g] - parts[2 - g] for g in range(3)],
            axis=0,
        )

    def product(parts, table_hi, table_lo):
        high, low = split(folded(parts))
        both = jnp.concatenate([high, low], axis=1)
        twice = jnp.concatenate([table_hi[...], table_hi[...]], axis=0)
        contract = ((1,), (0,))
        return wide_dot(both, twice, contract) + wide_dot(high, table_lo[...], contract)

    by_cos = product(even, cos_hi, cos_lo)
    by_sin = product(odd, sin_hi, sin_lo)
    real = jnp.zeros((24, 768), F32)
    imag = jnp.zeros((24, 768), F32)
    for g in range(3):
        plus = slice(24 * g, 24 * g + 24)
        minus = slice(72 + 24 * g, 96 + 24 * g)
        turn_cos = step_cos[4 + g : 5 + g]
        turn_sin = step_sin[4 + g : 5 + g]
        real = real + turn_cos * by_cos[plus] - turn_sin * by_sin[minus]
        imag = imag - turn_sin * by_cos[minus] - turn_cos * by_sin[plus]
    live = (2.0 * orders + 1.0 <= count).astype(F32) * (weight / count)
    centre_cos = step_cos[7:8] * live
    centre_sin = step_sin[7:8] * live
    both = (real * centre_cos + imag * centre_sin, imag * centre_cos - real * centre_sin)
    for t in range(6):
        for r in range(2):
            at = (t // 3) * 1728 + (t % 3) * 48 + r * 24
            spectra[pl.ds(at + pair * 144, 24), :] = both[r][:, 128 * t : 128 * t + 128]

    @pl.when(pair == 11)
    def _():
        for c in range(27):
            out[c] = spectra[128 * c : 128 * c + 128, :].T


def inverse_kernel(points, orders_ref, spectra_in, out, rows, spectra, cos_hi, cos_lo, sin_hi, sin_lo):
    pair = pl.program_id(0)

    @pl.when(pair == 0)
    def _():
        for c in range(27):
            spectra[128 * c : 128 * c + 128, :] = spectra_in[c].T

    count = points[0, pair].astype(F32)
    orders = orders_ref[...]
    fine_pair, step_pair = phase_rows(orders, count)
    fill_tables(fine_pair, step_pair, cos_hi, cos_lo, sin_hi, sin_lo)
    step_cos, step_sin = step_pair

    def part(r):
        return jnp.concatenate(
            [
                spectra[pl.ds((t // 3) * 1728 + (t % 3) * 48 + r * 24 + pair * 144, 24), :]
                for t in range(6)
            ],
            axis=1,
        )

    in_real, in_imag = part(0), part(1)
    live = 2.0 * orders + 1.0 <= count
    doubling = jnp.where(live, jnp.where(orders < 0.5, 1.0, 2.0), 0.0)
    centre_cos = step_cos[7:8] * doubling
    centre_sin = step_sin[7:8] * doubling
    real = in_real * centre_cos - in_imag * centre_sin
    imag = in_real * centre_sin + in_imag * centre_cos

    def turned(first, second):
        return jnp.concatenate(
            [first * step_cos[4 + g : 5 + g] for g in range(3)]
            + [second * step_sin[4 + g : 5 + g] for g in range(3)],
            axis=0,
        )

    def product(first, second, table_hi, table_lo):
        high, low = split(turned(first, second))
        contract = ((1,), (1,))
        both = wide_dot(high, jnp.concatenate([table_hi[...], table_lo[...]], axis=0), contract)
        return both[:, :128] + both[:, 128:] + wide_dot(low, table_hi[...], contract)

    by_cos = product(real, imag, cos_hi, cos_lo)
    by_sin = product(imag, real, sin_hi, sin_lo)
    place = lax.broadcasted_iota(jnp.int32, (24, 128), 1).astype(F32)

    def put(block, value):
        rows[:, 128 * block : 128 * block + 128] = jnp.where(place + 128.0 * block < count, value, 0.0)

    for g in range(3):
        c1, c2 = by_cos[24 * g : 24 * g + 24], by_cos[72 + 24 * g : 96 + 24 * g]
        s1, s2 = by_sin[24 * g : 24 * g + 24], by_sin[72 + 24 * g : 96 + 24 * g]
        minus, plus = c1 - c2, c1 + c2
        total, differ = s1 + s2, s1 - s2
        put(2 * (3 + g) + 1, minus - total)
        put(2 * (3 + g), reversed_lanes(minus + total))
        put(2 * (2 - g) + 1, plus - differ)
        put(2 * (2 - g), reversed_lanes(plus + differ))
    for f in range(3):
        for l in range(4):
            at = 8 * f + 2 * l
            out[f, l, 0] = rows[at : at + 2, :]


def block_swap(parts):
    lane = lax.broadcasted_iota(jnp.int32, parts[0].shape, 1)
    far = lane < 64
    near = (lane // 32) % 2 == 0
    a, b, c, d = parts
    a, c = jnp.where(far, a, pltpu.roll(c, 64, 1)), jnp.where(far, pltpu.roll(a, 64, 1), c)
    b, d = jnp.where(far, b, pltpu.roll(d, 64, 1)), jnp.where(far, pltpu.roll(b, 64, 1), d)
    a, b = jnp.where(near, a, pltpu.roll(b, 32, 1)), jnp.where(near, pltpu.roll(a, 96, 1), b)
    c, d = jnp.where(near, c, pltpu.roll(d, 32, 1)), jnp.where(near, pltpu.roll(c, 96, 1), d)
    return a, b, c, d


def hemispheres(value):
    row = lax.broadcasted_iota(jnp.int32, value.shape, 0)
    first = row % 2 == 0
    n = value.shape[0]
    other = jnp.where(first, pltpu.roll(value, n - 1, 0), pltpu.roll(value, 1, 0))
    return other + jnp.where(first, value, -value)


def legendre_kernel(lowers, rates, legendre, arrived, out, flat, left, back, tiled, table_hi, table_lo):
    slot = pl.program_id(0)
    me = lax.axis_index("band") * 4 + lax.axis_index("lev")

    @pl.when(slot == 0)
    def _():
        for c in range(27):
            flat[128 * c : 128 * c + 128, :] = arrived[c].T

    def at(member, i, r, f):
        return member * 1728 + i * 144 + r * 24 + f * 8

    for c in range(6):
        tiled[c] = legendre[0, :, 128 * c : 128 * c + 128]
    first_lane = lax.broadcasted_iota(jnp.int32, (384, 128), 1) == 0
    tiled[6] = jnp.where(first_lane, legendre[0, :, 768:769], 0.0)
    for i in range(12):
        for c in range(7):
            high, low = split(tiled[c, pl.ds(i, 32, stride=12), :])
            table_hi[32 * i : 32 * i + 32, 128 * c : 128 * c + 128] = high
            table_lo[32 * i : 32 * i + 32, 128 * c : 128 * c + 128] = low
    for member in range(2):
        for r in range(2):
            for f in range(3):
                for g in range(3):
                    parts = [flat[pl.ds(at(member, 4 * g + k, r, f) + slot * 48, 8), :] for k in range(4)]
                    for z, value in enumerate(block_swap(parts)):
                        row = ((member * 2 + r) * 4 + z) * 24 + f * 8
                        left[row : row + 8, 128 * g : 128 * g + 128] = hemispheres(value)
    lower = lowers[slot, me].astype(F32)
    column = lax.broadcasted_iota(jnp.int32, (8, 896), 1).astype(F32)
    row = lax.broadcasted_iota(jnp.int32, (8, 896), 0)
    second = column >= 768.0 - lower
    degree = jnp.where(second, column - 1.0, lower + column)
    order = jnp.where(second, 767.0 - lower, lower)
    gap = degree - order
    odd = gap - 2.0 * jnp.floor(gap * 0.5)
    wanted = jnp.where(row % 2 == 0, 1.0 - odd, odd)
    ratio = degree * (degree + 1.0) / float(767 * 768)
    square = ratio * ratio
    for member in range(2):
        kept = jnp.where(second, 1.0, 0.0) if member else jnp.where(second, 0.0, 1.0)
        kept = kept * wanted
        for r in range(2):
            top = (member * 2 + r) * 96
            value = left[top : top + 96, :]
            high, low = split(value)
            contract = ((1,), (0,))
            coef = wide_dot(high, table_hi[...], contract) + wide_dot(high, table_lo[...], contract)
            coef = coef + wide_dot(low, table_hi[...], contract)
            scale = jnp.concatenate([kept / (1.0 + rates[8 * k : 8 * k + 8, :] * square) for k in range(12)], axis=0)
            damped = coef * scale
            high, low = split(damped)
            contract = ((1,), (1,))
            given = wide_dot(high, table_hi[...], contract) + wide_dot(high, table_lo[...], contract)
            given = given + wide_dot(low, table_hi[...], contract)
            back[top : top + 96, :] = given
    for member in range(2):
        for r in range(2):
            for f in range(3):
                for g in range(3):
                    parts = []
                    for z in range(4):
                        row = ((member * 2 + r) * 4 + z) * 24 + f * 8
                        parts.append(hemispheres(back[row : row + 8, 128 * g : 128 * g + 128]))
                    for k, value in enumerate(block_swap(parts)):
                        flat[pl.ds(at(member, 4 * g + k, r, f) + slot * 48, 8), :] = value

    @pl.when(slot == 2)
    def _():
        for c in range(27):
            out[c] = flat[128 * c : 128 * c + 128, :].T


def exchange_kernel(forward, source, out, held, got, send_sem, recv_sem, local_sem):
    band, lev = lax.axis_index("band"), lax.axis_index("lev")
    me = band * 4 + lev
    barrier = pltpu.get_barrier_semaphore()

    def peer(k):
        t = lax.rem(me + k, 128)
        return t, t // 4, lax.rem(t, 4)

    def greet(k, carry):
        _, b, z = peer(k)
        pl.semaphore_signal(barrier, inc=1, device_id=(b, z), device_id_type=MESH)
        return carry

    load = pltpu.make_async_copy(source, held, local_sem)
    load.start()
    lax.fori_loop(1, 128, greet, 0)
    mine_device, mine_grid = me, lev * 32 + band
    load.wait()
    here = (mine_device, mine_grid) if forward else (mine_grid, mine_device)
    got[:, pl.ds(here[1], 1), :] = held[:, pl.ds(here[0], 1), :]
    pl.semaphore_wait(barrier, 127)

    def copy(k):
        t, b, z = peer(k)
        grid = z * 32 + b
        row, place = (t, mine_grid) if forward else (grid, mine_device)
        return pltpu.make_async_remote_copy(
            src_ref=held.at[:, pl.ds(row, 1), :],
            dst_ref=got.at[:, pl.ds(place, 1), :],
            send_sem=send_sem,
            recv_sem=recv_sem,
            device_id=(b, z),
            device_id_type=MESH,
        )

    def begin(k, carry):
        copy(k).start()
        return carry

    lax.fori_loop(1, 128, begin, 0)
    everything = pltpu.make_async_remote_copy(
        src_ref=held.at[:, pl.ds(0, 127), :],
        dst_ref=got.at[:, pl.ds(0, 127), :],
        send_sem=send_sem,
        recv_sem=recv_sem,
        device_id=(band, lev),
        device_id_type=MESH,
    )
    everything.wait()
    store = pltpu.make_async_copy(got, out, local_sem)
    store.start()
    store.wait()


BLOCKS = jax.ShapeDtypeStruct((27, 128, 128), F32)
ANYWHERE = pl.BlockSpec(memory_space=pl.ANY)
SCALARS = pl.BlockSpec(memory_space=pltpu.SMEM)


def exchange(value, forward):
    return pl.pallas_call(
        functools.partial(exchange_kernel, forward),
        out_shape=BLOCKS,
        in_specs=[ANYWHERE],
        out_specs=ANYWHERE,
        scratch_shapes=[
            pltpu.VMEM((27, 128, 128), F32),
            pltpu.VMEM((27, 128, 128), F32),
            pltpu.SemaphoreType.DMA,
            pltpu.SemaphoreType.DMA,
            pltpu.SemaphoreType.DMA,
        ],
        compiler_params=pltpu.CompilerParams(collective_id=0 if forward else 1, has_side_effects=True),
        name="exchange_out" if forward else "exchange_back",
    )(value)


TABLES = [pltpu.VMEM((128, 768), BF16) for _ in range(4)]
GRID_BLOCK = pl.BlockSpec((3, 4, 1, 2, 1536), lambda i: (0, 0, i, 0, 0))
WHOLE = pl.BlockSpec((27, 128, 128), lambda i: (0, 0, 0))


def forward_part(points, weights, orders, field_grid, increment):
    return pl.pallas_call(
        forward_kernel,
        grid=(12,),
        out_shape=BLOCKS,
        in_specs=[SCALARS, SCALARS, pl.BlockSpec((1, 768), lambda i: (0, 0)), GRID_BLOCK, GRID_BLOCK],
        out_specs=WHOLE,
        scratch_shapes=[pltpu.VMEM((24, 1536), F32), pltpu.VMEM((3456, 128), F32)] + TABLES,
        name="forward",
    )(points, weights, orders, field_grid, increment)


def inverse_part(points, orders, spectra):
    return pl.pallas_call(
        inverse_kernel,
        grid=(12,),
        out_shape=jax.ShapeDtypeStruct((3, 4, 12, 2, 1536), F32),
        in_specs=[SCALARS, pl.BlockSpec((1, 768), lambda i: (0, 0)), WHOLE],
        out_specs=GRID_BLOCK,
        scratch_shapes=[pltpu.VMEM((24, 1536), F32), pltpu.VMEM((3456, 128), F32)] + TABLES,
        name="inverse",
    )(points, orders, spectra)


def legendre_part(lowers, rates, legendre, arrived):
    return pl.pallas_call(
        legendre_kernel,
        grid=(3,),
        out_shape=BLOCKS,
        in_specs=[
            SCALARS,
            pl.BlockSpec((96, 1), lambda i: (0, 0)),
            pl.BlockSpec((1, 384, 769), lambda i: (i, 0, 0)),
            WHOLE,
        ],
        out_specs=WHOLE,
        scratch_shapes=[
            pltpu.VMEM((3456, 128), F32),
            pltpu.VMEM((384, 384), F32),
            pltpu.VMEM((384, 384), F32),
            pltpu.VMEM((7, 384, 128), F32),
            pltpu.VMEM((384, 896), BF16),
            pltpu.VMEM((384, 896), BF16),
        ],
        name="legendre",
    )(lowers, rates, legendre, arrived)


def body(field_grid, increment, points, weights, pair_slot, legendre, strength):
    slots = 3 * lax.broadcasted_iota(jnp.int32, (3, 128, 1), 1) + lax.broadcasted_iota(jnp.int32, (3, 128, 1), 0)
    waves = lax.broadcasted_iota(jnp.int32, (1, 1, 384), 2)
    lowers = jnp.sum(jnp.where(pair_slot[None, None, :] == slots, waves, 0), axis=2)
    orders = jnp.concatenate([lowers.reshape(1, 384), 767 - lowers.reshape(1, 384)], axis=1).astype(F32)
    rates = strength.reshape(3, 4, 4).transpose(1, 0, 2)
    rates = jnp.broadcast_to(rates[..., None], (4, 3, 4, 2)).reshape(96, 1)
    counts = points.reshape(1, 12)
    sent = forward_part(counts, weights, orders, field_grid, increment)
    arrived = exchange(sent, True)
    given = legendre_part(lowers, rates, legendre, arrived)
    home = exchange(given, False)
    return inverse_part(counts, orders, home)


def solution(mesh):
    return jax.shard_map(
        body,
        mesh=mesh,
        in_specs=(
            P(None, "lev", "band", None, None),
            P(None, "lev", "band", None, None),
            P("band"),
            P(),
            P(),
            P(("band", "lev"), None, None),
            P(),
        ),
        out_specs=P(None, "lev", "band", None, None),
        check_vma=False,
    )
```

```python
import math

import jax
import jax.numpy as jnp
from jax import lax
from jax.experimental import pallas as pl
from jax.experimental.pallas import tpu as pltpu
from jax.sharding import PartitionSpec as P

MESH = pl.DeviceIdType.MESH
F32 = jnp.float32
BF16 = jnp.bfloat16
SIN_COEFS = [(-1) ** k * math.pi ** (2 * k + 1) / math.factorial(2 * k + 1) for k in range(7)]
COS_COEFS = [(-1) ** k * math.pi ** (2 * k) / math.factorial(2 * k) for k in range(8)]


def half_turn_pair(half):
    square = half * half
    sine = jnp.full_like(square, SIN_COEFS[-1])
    for coef in SIN_COEFS[-2::-1]:
        sine = sine * square + coef
    cosine = jnp.full_like(square, COS_COEFS[-1])
    for coef in COS_COEFS[-2::-1]:
        cosine = cosine * square + coef
    return cosine, sine * half


def turn_pair(orders, doubled, count):
    period = 2.0 * count
    product = orders * doubled
    rest = product - jnp.round(product / period) * period
    cosine, sine = half_turn_pair(rest / period)
    return 1.0 - 2.0 * sine * sine, 2.0 * sine * cosine


def split(value):
    high = value.astype(BF16)
    return high, (value - high.astype(F32)).astype(BF16)


def wide_dot(left, right, contract):
    return lax.dot_general(left, right, (contract, ((), ())), preferred_element_type=F32)


def phase_rows(orders, count):
    row = lax.broadcasted_iota(jnp.int32, (8, orders.shape[1]), 0)
    fine = 2 * row + 1
    step = jnp.where(row < 4, jnp.left_shift(16, jnp.minimum(row, 4)), (row - 4) * 512 + 256)
    step = jnp.where(row == 7, 1535, step)
    wide = jnp.broadcast_to(orders, (8, orders.shape[1]))
    fine_pair = turn_pair(wide, fine.astype(F32), count)
    step_pair = turn_pair(wide, step.astype(F32), count)
    return fine_pair, step_pair


def fill_tables(fine_pair, step_pair, tables):
    cos_hi, cos_lo, sin_hi, sin_lo = tables
    cosine, sine = fine_pair
    step_cos, step_sin = step_pair
    for level in range(4):
        turn_cos = step_cos[level : level + 1]
        turn_sin = step_sin[level : level + 1]
        next_cos = cosine * turn_cos - sine * turn_sin
        next_sin = sine * turn_cos + cosine * turn_sin
        cosine = jnp.concatenate([cosine, next_cos], axis=0)
        sine = jnp.concatenate([sine, next_sin], axis=0)
    high, low = split(cosine)
    cos_hi[...] = high
    cos_lo[...] = low
    high, low = split(sine)
    sin_hi[...] = high
    sin_lo[...] = low


def reversed_lanes(value):
    index = 127 - lax.broadcasted_iota(jnp.int32, value.shape, 1)
    return jnp.take_along_axis(value, index, axis=1)


def block_swap(parts):
    lane = lax.broadcasted_iota(jnp.int32, parts[0].shape, 1)
    far = lane < 64
    near = (lane // 32) % 2 == 0
    a, b, c, d = parts
    a, c = jnp.where(far, a, pltpu.roll(c, 64, 1)), jnp.where(far, pltpu.roll(a, 64, 1), c)
    b, d = jnp.where(far, b, pltpu.roll(d, 64, 1)), jnp.where(far, pltpu.roll(b, 64, 1), d)
    a, b = jnp.where(near, a, pltpu.roll(b, 32, 1)), jnp.where(near, pltpu.roll(a, 96, 1), b)
    c, d = jnp.where(near, c, pltpu.roll(d, 32, 1)), jnp.where(near, pltpu.roll(c, 96, 1), d)
    return a, b, c, d


def greet_all(barrier, me):
    def greet(k, carry):
        t = lax.rem(me + k, 128)
        pl.semaphore_signal(barrier, inc=1, device_id=(t // 4, lax.rem(t, 4)), device_id_type=MESH)
        return carry

    lax.fori_loop(1, 128, greet, 0)


def partner(k, band, lev):
    step = lax.rem(k * 37, 128)
    y = lax.rem(band // 8 + step // 32, 4)
    x = lax.rem(band // 2 + step // 8, 4)
    core = lax.rem(band + step // 4, 2)
    return y * 8 + x * 2 + core, lax.rem(lev + step, 4)


LIGHT = 15
LOWER = 14
UPPER = 27 - LOWER
HEAVY_DEVICES = (32 - LIGHT) * 4


def post(source, target, chunks, row, place, sems, device):
    pltpu.make_async_remote_copy(
        src_ref=source.at[chunks, pl.ds(row, 1), :],
        dst_ref=target.at[chunks, pl.ds(place, 1), :],
        send_sem=sems.at[0],
        recv_sem=sems.at[1],
        device_id=device,
        device_id_type=MESH,
    ).start()


def drained(source, target, chunks, count, sem, sending, device):
    copy = pltpu.make_async_remote_copy(
        src_ref=source.at[chunks, pl.ds(0, count), :],
        dst_ref=target.at[chunks, pl.ds(0, count), :],
        send_sem=sem,
        recv_sem=sem,
        device_id=device,
        device_id_type=MESH,
    )
    if sending:
        copy.wait_send()
    else:
        copy.wait_recv()


LOW = pl.ds(0, LOWER)
HIGH = pl.ds(LOWER, UPPER)


def wave_orders(pair_slot):
    lanes = jnp.broadcast_to(pair_slot.astype(F32), (128, 384))
    column = jnp.concatenate([lanes[:, 128 * c : 128 * c + 128].T for c in range(3)], axis=0)
    wave = lax.broadcasted_iota(jnp.int32, (384, 128), 0).astype(F32)
    lane = lax.broadcasted_iota(jnp.int32, (384, 128), 1).astype(F32)
    lower = [jnp.sum(jnp.where(column == 3.0 * lane + s, wave, 0.0), axis=0, keepdims=True) for s in range(3)]
    lower = jnp.concatenate(lower, axis=1)
    return jnp.concatenate([lower, 767.0 - lower], axis=1)


def rows_at(member, r, pair, f=0, slot=0):
    return pl.multiple_of(member * 1728 + r * 24 + f * 8 + pair * 144 + slot * 48, 8)


def forward_tables(orders, count, tables):
    fine_pair, step_pair = phase_rows(orders, count)
    fill_tables(fine_pair, step_pair, tables)
    return step_pair


def forward_pair(field, increment, pair, count, weight, orders, tables, steps_ref, rows, spectra):
    for f in range(3):
        for l in range(4):
            at = 8 * f + 2 * l
            rows[at : at + 2, :] = field[f, l, pair] + increment[f, l, pair]
    step_cos, step_sin = forward_tables(orders, count, tables)
    steps_ref[0] = step_cos
    steps_ref[1] = step_sin
    cos_hi, cos_lo, sin_hi, sin_lo = tables
    value = rows[...]
    place = lax.broadcasted_iota(jnp.int32, value.shape, 1).astype(F32)
    value = jnp.where(place < count, value, 0.0)
    even, odd = [], []
    for block in range(6):
        low = reversed_lanes(value[:, 256 * block : 256 * block + 128])
        high = value[:, 256 * block + 128 : 256 * block + 256]
        even.append(high + low)
        odd.append(high - low)

    def folded(parts):
        return jnp.concatenate(
            [parts[3 + g] + parts[2 - g] for g in range(3)] + [parts[3 + g] - parts[2 - g] for g in range(3)],
            axis=0,
        )

    def product(parts, table_hi, table_lo):
        high, low = split(folded(parts))
        both = jnp.concatenate([high, low], axis=1)
        twice = jnp.concatenate([table_hi[...], table_hi[...]], axis=0)
        contract = ((1,), (0,))
        return wide_dot(both, twice, contract) + wide_dot(high, table_lo[...], contract)

    by_cos = product(even, cos_hi, cos_lo)
    by_sin = product(odd, sin_hi, sin_lo)
    real = jnp.zeros((24, 768), F32)
    imag = jnp.zeros((24, 768), F32)
    for g in range(3):
        plus = slice(24 * g, 24 * g + 24)
        minus = slice(72 + 24 * g, 96 + 24 * g)
        turn_cos = step_cos[4 + g : 5 + g]
        turn_sin = step_sin[4 + g : 5 + g]
        real = real + turn_cos * by_cos[plus] - turn_sin * by_sin[minus]
        imag = imag - turn_sin * by_cos[minus] - turn_cos * by_sin[plus]
    live = (2.0 * orders + 1.0 <= count).astype(F32) * (weight / count)
    centre_cos = step_cos[7:8] * live
    centre_sin = step_sin[7:8] * live
    both = (real * centre_cos + imag * centre_sin, imag * centre_cos - real * centre_sin)
    for t in range(6):
        for r in range(2):
            spectra[pl.ds(rows_at(t // 3, r, pair, 0, t % 3), 24), :] = both[r][:, 128 * t : 128 * t + 128]


def inverse_pair(spectra, pair, count, orders, tables, steps_ref, rows, out):
    cos_hi, cos_lo, sin_hi, sin_lo = tables
    step_cos, step_sin = steps_ref[0], steps_ref[1]

    def part(r):
        return jnp.concatenate(
            [spectra[pl.ds(rows_at(t // 3, r, pair, 0, t % 3), 24), :] for t in range(6)], axis=1
        )

    in_real, in_imag = part(0), part(1)
    live = 2.0 * orders + 1.0 <= count
    doubling = jnp.where(live, jnp.where(orders < 0.5, 1.0, 2.0), 0.0)
    centre_cos = step_cos[7:8] * doubling
    centre_sin = step_sin[7:8] * doubling
    real = in_real * centre_cos - in_imag * centre_sin
    imag = in_real * centre_sin + in_imag * centre_cos

    def turned(first, second):
        return jnp.concatenate(
            [first * step_cos[4 + g : 5 + g] for g in range(3)]
            + [second * step_sin[4 + g : 5 + g] for g in range(3)],
            axis=0,
        )

    def product(first, second, table_hi, table_lo):
        high, low = split(turned(first, second))
        contract = ((1,), (1,))
        both = wide_dot(high, jnp.concatenate([table_hi[...], table_lo[...]], axis=0), contract)
        return both[:, :128] + both[:, 128:] + wide_dot(low, table_hi[...], contract)

    by_cos = product(real, imag, cos_hi, cos_lo)
    by_sin = product(imag, real, sin_hi, sin_lo)
    place = lax.broadcasted_iota(jnp.int32, (24, 128), 1).astype(F32)

    def put(block, value):
        rows[:, 128 * block : 128 * block + 128] = jnp.where(place + 128.0 * block < count, value, 0.0)

    for g in range(3):
        c1, c2 = by_cos[24 * g : 24 * g + 24], by_cos[72 + 24 * g : 96 + 24 * g]
        s1, s2 = by_sin[24 * g : 24 * g + 24], by_sin[72 + 24 * g : 96 + 24 * g]
        minus, plus = c1 - c2, c1 + c2
        total, differ = s1 + s2, s1 - s2
        put(2 * (3 + g) + 1, minus - total)
        put(2 * (3 + g), reversed_lanes(minus + total))
        put(2 * (2 - g) + 1, plus - differ)
        put(2 * (2 - g), reversed_lanes(plus + differ))
    for f in range(3):
        for l in range(4):
            at = 8 * f + 2 * l
            out[f, l, pair] = rows[at : at + 2, :]


def prepare_legendre(slot, source, by_lat, by_wave, table_hi, table_lo, last):
    for t in range(3):
        by_lat[t] = source[slot, 0:768, 128 * t : 128 * t + 128]
    for t in range(3):
        for parity in range(2):
            for c in range(3):
                chunk = by_lat[t, pl.ds(256 * c + parity, 128, stride=2), :]
                by_wave[3 * parity + c, 128 * t : 128 * t + 128, :] = chunk.T
        final = jnp.broadcast_to(source[slot, 768:769, 128 * t : 128 * t + 128], (128, 128))
        by_wave[6, 128 * t : 128 * t + 128, :] = final.T
    for i in range(12):
        for c in range(6):
            high, low = split(by_wave[c, pl.ds(i, 32, stride=12), :])
            table_hi[slot, 32 * i : 32 * i + 32, 128 * c : 128 * c + 128] = high
            table_lo[slot, 32 * i : 32 * i + 32, 128 * c : 128 * c + 128] = low
    for t in range(3):
        column = jnp.concatenate([by_wave[6, pl.ds(4 * t + k, 32, stride=12), :] for k in range(4)], axis=0)
        last[slot, :, 128 * t : 128 * t + 128] = column.T[0:8]


def legendre_slot(slot, lower, rates, flat, left, back, table_hi, table_lo, last):
    row = lax.broadcasted_iota(jnp.int32, (8, 128), 0)
    first = row % 2 == 0
    half_lower = lower * 0.5
    odd_lower = lower - 2.0 * jnp.floor(half_lower) > 0.5
    for member in range(2):
        for r in range(2):
            for f in range(3):
                for g in range(3):
                    parts = [flat[pl.ds(rows_at(member, r, 4 * g + k, f, slot), 8), :] for k in range(4)]
                    swapped = block_swap(parts)
                    for z in range(2):
                        a, b = swapped[2 * z], swapped[2 * z + 1]
                        north = jnp.where(first, a, pltpu.roll(b, 1, 0))
                        south = jnp.where(first, pltpu.roll(a, 7, 0), b)
                        plus, minus = north + south, north - south
                        if member:
                            plus, minus = jnp.where(odd_lower, minus, plus), jnp.where(odd_lower, plus, minus)
                        at = (((member * 2 + r) * 2 + z) * 3 + f) * 8
                        left[0, at : at + 8, 128 * g : 128 * g + 128] = plus
                        left[1, at : at + 8, 128 * g : 128 * g + 128] = minus
    lower_row = jnp.concatenate([lower[0:1]] * 3, axis=1)
    for parity in range(2):
        value = left[parity]
        high, low = split(value)
        both = jnp.concatenate([high, low], axis=1)
        cols = slice(384 * parity, 384 * parity + 384)
        hi_table = table_hi[slot, :, cols]
        lo_table = table_lo[slot, :, cols]
        contract = ((1,), (0,))
        coef = wide_dot(both, jnp.concatenate([hi_table, hi_table], axis=0), contract)
        coef = coef + wide_dot(high, lo_table, contract)
        column = 2.0 * lax.broadcasted_iota(jnp.int32, (1, 384), 1).astype(F32) + float(parity)
        second = column >= 768.0 - lower_row
        scales = []
        for member in range(2):
            degree = column - 1.0 if member else lower_row + column
            kept = jnp.where(second, 1.0, 0.0) if member else jnp.where(second, 0.0, 1.0)
            ratio = degree * (degree + 1.0) / float(767 * 768)
            square = ratio * ratio
            scale = jnp.concatenate([kept / (1.0 + rate * square) for rate in rates], axis=0)
            scales += [scale, scale]
        damped = coef * jnp.concatenate(scales, axis=0)
        high, low = split(damped)
        both = jnp.concatenate([high, low], axis=1)
        contract = ((1,), (1,))
        given = wide_dot(both, jnp.concatenate([hi_table, hi_table], axis=1), contract)
        given = given + wide_dot(high, lo_table, contract)
        if parity == 0:
            final = last[slot, 0:1, :]
            extra = jnp.sum(value[96:192] * final, axis=1, keepdims=True)
            fade = jnp.concatenate([1.0 / (1.0 + rate) for rate in rates] * 2, axis=0)
            back[parity, 0:96, :] = given[0:96]
            back[parity, 96:192, :] = given[96:192] + (extra * fade) * final
        else:
            back[parity] = given
    for member in range(2):
        for r in range(2):
            for f in range(3):
                for g in range(3):
                    parts = []
                    for z in range(2):
                        at = (((member * 2 + r) * 2 + z) * 3 + f) * 8
                        plus = back[0, at : at + 8, 128 * g : 128 * g + 128]
                        minus = back[1, at : at + 8, 128 * g : 128 * g + 128]
                        if member:
                            plus, minus = jnp.where(odd_lower, minus, plus), jnp.where(odd_lower, plus, minus)
                        north, south = plus + minus, plus - minus
                        parts.append(jnp.where(first, north, pltpu.roll(south, 1, 0)))
                        parts.append(jnp.where(first, pltpu.roll(north, 7, 0), south))
                    for k, value in enumerate(block_swap(parts)):
                        flat[pl.ds(rows_at(member, r, 4 * g + k, f, slot), 8), :] = value


def step_kernel(
    points, weights, strength, pair_slot, field_hbm, increment_hbm, legendre_hbm, out_hbm,
    field, increment, source, waves, steps, rows, flat, sent, got, left, back, by_lat, by_wave, table_hi, table_lo, last,
    cos_hi_a, cos_lo_a, sin_hi_a, sin_lo_a, cos_hi_b, cos_lo_b, sin_hi_b, sin_lo_b,
    load_sems, low_sems, high_sems, store_sem,
):
    band, lev = lax.axis_index("band"), lax.axis_index("lev")
    me = band * 4 + lev
    here = lev * 32 + band
    device = (band, lev)
    light = band < LIGHT
    loads = [
        pltpu.make_async_copy(field_hbm, field, load_sems.at[0]),
        pltpu.make_async_copy(increment_hbm, increment, load_sems.at[1]),
        pltpu.make_async_copy(legendre_hbm, source, load_sems.at[2]),
    ]
    for load in loads:
        load.start()
    for z in range(4):
        got[0, LOWER:27, 32 * z : 32 * z + LIGHT, :] = jnp.zeros((UPPER, LIGHT, 128), F32)

    @pl.when(light)
    def _():
        got[1, LOWER:27, :, :] = jnp.zeros((UPPER, 128, 128), F32)

    barrier = pltpu.get_barrier_semaphore()
    greet_all(barrier, me)
    waves[...] = wave_orders(pair_slot[...])
    loads[0].wait()
    loads[1].wait()
    table_sets = ((cos_hi_a, cos_lo_a, sin_hi_a, sin_lo_a), (cos_hi_b, cos_lo_b, sin_hi_b, sin_lo_b))

    def forward(k, carry):
        for side in range(2):
            pair = 2 * k + side
            forward_pair(
                field, increment, pair, points[pair].astype(F32), weights[band * 12 + pair], waves[...],
                [table.at[k] for table in table_sets[side]], steps.at[side, k], rows.at[side], flat,
            )
        return carry

    lax.fori_loop(0, 6, forward, 0)
    for c in range(27):
        sent[0, c] = flat[128 * c : 128 * c + 128, :].T
    pl.semaphore_wait(barrier, 127)

    def send_out(k, carry):
        b, z = partner(k, band, lev)
        post(sent.at[0], got.at[0], LOW, b * 4 + z, here, low_sems.at[0], (b, z))

        @pl.when(band >= LIGHT)
        def _():
            post(sent.at[0], got.at[0], HIGH, b * 4 + z, here, high_sems.at[0], (b, z))

        return carry

    lax.fori_loop(1, 128, send_out, 0)
    got[0, :, pl.ds(here, 1), :] = sent[0, :, pl.ds(me, 1), :]
    loads[2].wait()

    def prepare(slot, carry):
        prepare_legendre(slot, source, by_lat, by_wave, table_hi, table_lo, last)
        return carry

    lax.fori_loop(0, 3, prepare, 0)
    rates = []
    for z in range(2):
        for f in range(3):
            index = lax.broadcasted_iota(jnp.int32, (8, 1), 0)
            rate = jnp.zeros((8, 1), F32)
            for l in range(4):
                for side in range(2):
                    rate = jnp.where(index == 2 * l + side, strength[f, 4 * (2 * z + side) + l], rate)
            rates.append(rate)
    drained(sent.at[0], got.at[0], LOW, 127, low_sems.at[0, 1], False, device)

    @pl.when(light)
    def _():
        drained(sent.at[0], got.at[0], HIGH, HEAVY_DEVICES, high_sems.at[0, 1], False, device)

    @pl.when(band >= LIGHT)
    def _():
        drained(sent.at[0], got.at[0], HIGH, HEAVY_DEVICES - 1, high_sems.at[0, 1], False, device)

    for c in range(27):
        flat[128 * c : 128 * c + 128, :] = got[0, c].T
    slots = pair_slot[...].astype(F32)

    def legendre(slot, carry):
        mine = (3 * me + slot).astype(F32)
        index = lax.broadcasted_iota(jnp.int32, (1, 384), 1).astype(F32)
        lower = jnp.sum(jnp.where(slots == mine, index, 0.0), axis=1, keepdims=True)
        lower = jnp.broadcast_to(lower, (8, 128))
        legendre_slot(slot, lower, rates, flat, left, back, table_hi, table_lo, last)
        return carry

    lax.fori_loop(0, 3, legendre, 0)
    for c in range(27):
        sent[1, c] = flat[128 * c : 128 * c + 128, :].T

    def send_back(k, carry):
        b, z = partner(k, band, lev)
        post(sent.at[1], got.at[1], LOW, z * 32 + b, me, low_sems.at[1], (b, z))

        @pl.when(b >= LIGHT)
        def _():
            post(sent.at[1], got.at[1], HIGH, z * 32 + b, me, high_sems.at[1], (b, z))

        return carry

    lax.fori_loop(1, 128, send_back, 0)
    got[1, 0:LOWER, pl.ds(me, 1), :] = sent[1, 0:LOWER, pl.ds(here, 1), :]

    @pl.when(band >= LIGHT)
    def _():
        got[1, LOWER:27, pl.ds(me, 1), :] = sent[1, LOWER:27, pl.ds(here, 1), :]
        drained(sent.at[0], got.at[0], HIGH, 127, high_sems.at[0, 0], True, device)

    drained(sent.at[0], got.at[0], LOW, 127, low_sems.at[0, 0], True, device)
    drained(sent.at[1], got.at[1], LOW, 127, low_sems.at[1, 1], False, device)

    @pl.when(band >= LIGHT)
    def _():
        drained(sent.at[1], got.at[1], HIGH, 127, high_sems.at[1, 1], False, device)

    for c in range(27):
        flat[128 * c : 128 * c + 128, :] = got[1, c].T

    def inverse(k, carry):
        for side in range(2):
            pair = 2 * k + side
            inverse_pair(
                flat, pair, points[pair].astype(F32), waves[...],
                [table.at[k] for table in table_sets[side]], steps.at[side, k], rows.at[side], field,
            )
        return carry

    lax.fori_loop(0, 6, inverse, 0)
    store = pltpu.make_async_copy(field, out_hbm, store_sem)
    store.start()
    drained(sent.at[1], got.at[1], LOW, 127, low_sems.at[1, 0], True, device)

    @pl.when(light)
    def _():
        drained(sent.at[1], got.at[1], HIGH, HEAVY_DEVICES, high_sems.at[1, 0], True, device)

    @pl.when(band >= LIGHT)
    def _():
        drained(sent.at[1], got.at[1], HIGH, HEAVY_DEVICES - 1, high_sems.at[1, 0], True, device)

    store.wait()


ANYWHERE = pl.BlockSpec(memory_space=pl.ANY)
SCALARS = pl.BlockSpec(memory_space=pltpu.SMEM)


def body(field_grid, increment, points, weights, pair_slot, legendre, strength):
    grid = (3, 4, 12, 2, 1536)
    return pl.pallas_call(
        step_kernel,
        out_shape=jax.ShapeDtypeStruct(grid, F32),
        in_specs=[SCALARS, SCALARS, SCALARS, pl.BlockSpec(memory_space=pltpu.VMEM), ANYWHERE, ANYWHERE, ANYWHERE],
        out_specs=ANYWHERE,
        scratch_shapes=[
            pltpu.VMEM(grid, F32),
            pltpu.VMEM(grid, F32),
            pltpu.VMEM((3, 769, 384), F32),
            pltpu.VMEM((1, 768), F32),
            pltpu.VMEM((2, 6, 2, 8, 768), F32),
            pltpu.VMEM((2, 24, 1536), F32),
            pltpu.VMEM((3456, 128), F32),
            pltpu.VMEM((2, 27, 128, 128), F32),
            pltpu.VMEM((2, 27, 128, 128), F32),
            pltpu.VMEM((2, 192, 384), F32),
            pltpu.VMEM((2, 192, 384), F32),
            pltpu.VMEM((3, 768, 128), F32),
            pltpu.VMEM((7, 384, 128), F32),
            pltpu.VMEM((3, 384, 768), BF16),
            pltpu.VMEM((3, 384, 768), BF16),
            pltpu.VMEM((3, 8, 384), F32),
        ]
        + [pltpu.VMEM((6, 128, 768), BF16) for _ in range(8)]
        + [
            pltpu.SemaphoreType.DMA((3,)),
            pltpu.SemaphoreType.DMA((2, 2)),
            pltpu.SemaphoreType.DMA((2, 2)),
            pltpu.SemaphoreType.DMA,
        ],
        compiler_params=pltpu.CompilerParams(
            collective_id=0, has_side_effects=True, vmem_limit_bytes=60 * 1024 * 1024
        ),
        name="spectral_step",
    )(points, weights, strength, pair_slot.reshape(1, 384), field_grid, increment, jnp.swapaxes(legendre, 1, 2))


def solution(mesh):
    return jax.shard_map(
        body,
        mesh=mesh,
        in_specs=(
            P(None, "lev", "band", None, None),
            P(None, "lev", "band", None, None),
            P("band"),
            P(),
            P(),
            P(("band", "lev"), None, None),
            P(),
        ),
        out_specs=P(None, "lev", "band", None, None),
        check_vma=False,
    )
```

```python
import math

import jax
import jax.numpy as jnp
from jax import lax
from jax.experimental import pallas as pl
from jax.experimental.pallas import tpu as pltpu
from jax.sharding import PartitionSpec as P

MESH = pl.DeviceIdType.MESH
F32 = jnp.float32
BF16 = jnp.bfloat16
SIN_COEFS = [(-1) ** k * math.pi ** (2 * k + 1) / math.factorial(2 * k + 1) for k in range(7)]
COS_COEFS = [(-1) ** k * math.pi ** (2 * k) / math.factorial(2 * k) for k in range(8)]


def half_turn_pair(half):
    square = half * half
    sine = jnp.full_like(square, SIN_COEFS[-1])
    for coef in SIN_COEFS[-2::-1]:
        sine = sine * square + coef
    cosine = jnp.full_like(square, COS_COEFS[-1])
    for coef in COS_COEFS[-2::-1]:
        cosine = cosine * square + coef
    return cosine, sine * half


def turn_pair(orders, doubled, count):
    period = 2.0 * count
    product = orders * doubled
    rest = product - jnp.round(product / period) * period
    cosine, sine = half_turn_pair(rest / period)
    return 1.0 - 2.0 * sine * sine, 2.0 * sine * cosine


def split(value):
    high = value.astype(BF16)
    return high, (value - high.astype(F32)).astype(BF16)


def wide_dot(left, right, contract):
    return lax.dot_general(left, right, (contract, ((), ())), preferred_element_type=F32)


def phase_rows(orders, count):
    row = lax.broadcasted_iota(jnp.int32, (8, orders.shape[1]), 0)
    fine = 2 * row + 1
    step = jnp.where(row < 4, jnp.left_shift(16, jnp.minimum(row, 4)), (row - 4) * 512 + 256)
    step = jnp.where(row == 7, 1535, step)
    wide = jnp.broadcast_to(orders, (8, orders.shape[1]))
    fine_pair = turn_pair(wide, fine.astype(F32), count)
    step_pair = turn_pair(wide, step.astype(F32), count)
    return fine_pair, step_pair


def fill_tables(fine_pair, step_pair, tables, index):
    cosine, sine = fine_pair
    step_cos, step_sin = step_pair
    for level in range(4):
        turn_cos = step_cos[level : level + 1]
        turn_sin = step_sin[level : level + 1]
        next_cos = cosine * turn_cos - sine * turn_sin
        next_sin = sine * turn_cos + cosine * turn_sin
        cosine = jnp.concatenate([cosine, next_cos], axis=0)
        sine = jnp.concatenate([sine, next_sin], axis=0)
    for n, value in enumerate((cosine, sine)):
        high, low = split(value)
        tables[(*index, 2 * n)] = high
        tables[(*index, 2 * n + 1)] = low


def reversed_lanes(value):
    index = 127 - lax.broadcasted_iota(jnp.int32, value.shape, 1)
    return jnp.take_along_axis(value, index, axis=1)


def block_swap(parts):
    lane = lax.broadcasted_iota(jnp.int32, parts[0].shape, 1)
    far = lane < 64
    near = (lane // 32) % 2 == 0
    a, b, c, d = parts
    a, c = jnp.where(far, a, pltpu.roll(c, 64, 1)), jnp.where(far, pltpu.roll(a, 64, 1), c)
    b, d = jnp.where(far, b, pltpu.roll(d, 64, 1)), jnp.where(far, pltpu.roll(b, 64, 1), d)
    a, b = jnp.where(near, a, pltpu.roll(b, 32, 1)), jnp.where(near, pltpu.roll(a, 96, 1), b)
    c, d = jnp.where(near, c, pltpu.roll(d, 32, 1)), jnp.where(near, pltpu.roll(c, 96, 1), d)
    return a, b, c, d


def greet_all(barrier, me):
    def greet(k, carry):
        t = lax.rem(me + k, 128)
        pl.semaphore_signal(barrier, inc=1, device_id=(t // 4, lax.rem(t, 4)), device_id_type=MESH)
        return carry

    lax.fori_loop(1, 128, greet, 0)


LIGHT = 15
ALL = 9
LOWER = 5
HEAVY = (32 - LIGHT) * 4
SIDES = 4


def chunks_of(slot, count):
    return pl.ds(ALL * slot, count)


def post(source, target, chunks, row, place, sems, device):
    pltpu.make_async_remote_copy(
        src_ref=source.at[chunks, pl.ds(row, 1), :],
        dst_ref=target.at[chunks, pl.ds(place, 1), :],
        send_sem=sems.at[0],
        recv_sem=sems.at[1],
        device_id=device,
        device_id_type=MESH,
    ).start()


def drained(ref, count, sem):
    pltpu.make_async_copy(ref.at[pl.ds(0, count), :], ref.at[pl.ds(0, count), :], sem).wait()


def to_everyone(band, lev, send):
    y, x, core = band // 8, (band // 2) % 4, band % 2
    cores = [core, 1 - core]
    levs = [lax.rem(lev + n, 4) for n in range(4)]

    def some(t, carry):
        ys = [lax.rem(y + lax.div(t, 4) + n, 4) for n in range(4)]
        xs = [lax.rem(x + lax.rem(t, 4) + n, 4) for n in range(4)]
        for n in range(8):
            b = ys[n % 4] * 8 + xs[n // 2] * 2 + cores[n // 4]
            z = levs[n % 4]
            if n == 0:

                @pl.when(t > 0)
                def _():
                    send(b, z)

            else:
                send(b, z)
        return carry

    lax.fori_loop(0, 16, some, 0)


def wave_orders(pair_slot):
    lanes = jnp.broadcast_to(pair_slot.astype(F32), (128, 384))
    column = jnp.concatenate([lanes[:, 128 * c : 128 * c + 128].T for c in range(3)], axis=0)
    wave = lax.broadcasted_iota(jnp.int32, (384, 128), 0).astype(F32)
    lane = lax.broadcasted_iota(jnp.int32, (384, 128), 1).astype(F32)
    lower = [jnp.sum(jnp.where(column == 3.0 * lane + s, wave, 0.0), axis=0, keepdims=True) for s in range(3)]
    return [jnp.concatenate([value, 767.0 - value], axis=1) for value in lower]


def rows_at(member, r, pair, f=0, slot=0):
    return pl.multiple_of(member * 576 + r * 24 + f * 8 + pair * 48 + slot * 1152, 8)


def fold_pair(field, increment, pair, count, rows, folds, index):
    for f in range(3):
        for l in range(4):
            at = 8 * f + 2 * l
            rows[at : at + 2, :] = field[f, l, pair] + increment[f, l, pair]
    value = rows[...]
    place = lax.broadcasted_iota(jnp.int32, value.shape, 1).astype(F32)
    value = jnp.where(place < count, value, 0.0)
    even, odd = [], []
    for block in range(6):
        low = reversed_lanes(value[:, 256 * block : 256 * block + 128])
        high = value[:, 256 * block + 128 : 256 * block + 256]
        even.append(high + low)
        odd.append(high - low)
    for n, parts in enumerate((even, odd)):
        whole = jnp.concatenate(
            [parts[3 + g] + parts[2 - g] for g in range(3)] + [parts[3 + g] - parts[2 - g] for g in range(3)],
            axis=0,
        )
        high, low = split(whole)
        folds[index, n, :, 0:128] = high
        folds[index, n, :, 128:256] = low


def forward_pair(slot, k, folds, pair, count, weight, orders, tables, steps, flat):
    fine_pair, step_pair = phase_rows(orders, count)
    fill_tables(fine_pair, step_pair, tables, (slot, k))
    step_cos, step_sin = step_pair
    steps[slot, k, 0] = step_cos
    steps[slot, k, 1] = step_sin

    def product(n):
        both = folds[k, n]
        table_hi, table_lo = tables[slot, k, 2 * n], tables[slot, k, 2 * n + 1]
        contract = ((1,), (0,))
        twice = jnp.concatenate([table_hi, table_hi], axis=0)
        return wide_dot(both, twice, contract) + wide_dot(both[:, 0:128], table_lo, contract)

    by_cos = product(0)
    by_sin = product(1)
    real = jnp.zeros((24, 256), F32)
    imag = jnp.zeros((24, 256), F32)
    for g in range(3):
        plus = slice(24 * g, 24 * g + 24)
        minus = slice(72 + 24 * g, 96 + 24 * g)
        turn_cos = step_cos[4 + g : 5 + g]
        turn_sin = step_sin[4 + g : 5 + g]
        real = real + turn_cos * by_cos[plus] - turn_sin * by_sin[minus]
        imag = imag - turn_sin * by_cos[minus] - turn_cos * by_sin[plus]
    live = (2.0 * orders + 1.0 <= count).astype(F32) * (weight / count)
    centre_cos = step_cos[7:8] * live
    centre_sin = step_sin[7:8] * live
    both = (real * centre_cos + imag * centre_sin, imag * centre_cos - real * centre_sin)
    for member in range(2):
        for r in range(2):
            flat[pl.ds(rows_at(member, r, pair, 0, slot), 24), :] = both[r][:, 128 * member : 128 * member + 128]


def inverse_pair(slot, k, flat, pair, count, orders, tables, steps, sums):
    step_cos, step_sin = steps[slot, k, 0], steps[slot, k, 1]

    def part(r):
        return jnp.concatenate(
            [flat[pl.ds(rows_at(member, r, pair, 0, slot), 24), :] for member in range(2)], axis=1
        )

    in_real, in_imag = part(0), part(1)
    live = 2.0 * orders + 1.0 <= count
    doubling = jnp.where(live, jnp.where(orders < 0.5, 1.0, 2.0), 0.0)
    centre_cos = step_cos[7:8] * doubling
    centre_sin = step_sin[7:8] * doubling
    real = in_real * centre_cos - in_imag * centre_sin
    imag = in_real * centre_sin + in_imag * centre_cos

    def turned(first, second):
        return jnp.concatenate(
            [first * step_cos[4 + g : 5 + g] for g in range(3)]
            + [second * step_sin[4 + g : 5 + g] for g in range(3)],
            axis=0,
        )

    def product(first, second, n):
        high, low = split(turned(first, second))
        contract = ((1,), (1,))
        table_hi, table_lo = tables[slot, k, 2 * n], tables[slot, k, 2 * n + 1]
        both = wide_dot(high, jnp.concatenate([table_hi, table_lo], axis=0), contract)
        return both[:, :128] + both[:, 128:] + wide_dot(low, table_hi, contract)

    by_cos = product(real, imag, 0)
    by_sin = product(imag, real, 1)
    sums[k, 0] = sums[k, 0] + by_cos
    sums[k, 1] = sums[k, 1] + by_sin


def unfold_pair(k, pair, count, sums, rows, out):
    by_cos, by_sin = sums[k, 0], sums[k, 1]
    place = lax.broadcasted_iota(jnp.int32, (24, 128), 1).astype(F32)

    def put(block, value):
        rows[:, 128 * block : 128 * block + 128] = jnp.where(place + 128.0 * block < count, value, 0.0)

    for g in range(3):
        c1, c2 = by_cos[24 * g : 24 * g + 24], by_cos[72 + 24 * g : 96 + 24 * g]
        s1, s2 = by_sin[24 * g : 24 * g + 24], by_sin[72 + 24 * g : 96 + 24 * g]
        minus, plus = c1 - c2, c1 + c2
        total, differ = s1 + s2, s1 - s2
        put(2 * (3 + g) + 1, minus - total)
        put(2 * (3 + g), reversed_lanes(minus + total))
        put(2 * (2 - g) + 1, plus - differ)
        put(2 * (2 - g), reversed_lanes(plus + differ))
    for f in range(3):
        for l in range(4):
            at = 8 * f + 2 * l
            out[f, l, pair] = rows[at : at + 2, :]


def prepare_legendre(slot, source, by_lat, by_wave, table_hi, table_lo, last):
    for t in range(3):
        by_lat[t] = source[slot, 0:768, 128 * t : 128 * t + 128]
    for t in range(3):
        for parity in range(2):
            for c in range(3):
                chunk = by_lat[t, pl.ds(256 * c + parity, 128, stride=2), :]
                by_wave[3 * parity + c, 128 * t : 128 * t + 128, :] = chunk.T
        final = jnp.broadcast_to(source[slot, 768:769, 128 * t : 128 * t + 128], (128, 128))
        by_wave[6, 128 * t : 128 * t + 128, :] = final.T
    for i in range(12):
        for c in range(6):
            high, low = split(by_wave[c, pl.ds(i, 32, stride=12), :])
            table_hi[slot, 32 * i : 32 * i + 32, 128 * c : 128 * c + 128] = high
            table_lo[slot, 32 * i : 32 * i + 32, 128 * c : 128 * c + 128] = low
    for t in range(3):
        column = jnp.concatenate([by_wave[6, pl.ds(4 * t + k, 32, stride=12), :] for k in range(4)], axis=0)
        last[slot, :, 128 * t : 128 * t + 128] = column.T[0:8]


def legendre_slot(slot, lower, rates, flat, left, back, table_hi, table_lo, last):
    row = lax.broadcasted_iota(jnp.int32, (8, 128), 0)
    first = row % 2 == 0
    half_lower = lower * 0.5
    odd_lower = lower - 2.0 * jnp.floor(half_lower) > 0.5
    for member in range(2):
        for r in range(2):
            for f in range(3):
                for g in range(3):
                    parts = [flat[pl.ds(rows_at(member, r, 4 * g + k, f, slot), 8), :] for k in range(4)]
                    swapped = block_swap(parts)
                    for z in range(2):
                        a, b = swapped[2 * z], swapped[2 * z + 1]
                        north = jnp.where(first, a, pltpu.roll(b, 1, 0))
                        south = jnp.where(first, pltpu.roll(a, 7, 0), b)
                        plus, minus = north + south, north - south
                        if member:
                            plus, minus = jnp.where(odd_lower, minus, plus), jnp.where(odd_lower, plus, minus)
                        at = (((member * 2 + r) * 2 + z) * 3 + f) * 8
                        left[0, at : at + 8, 128 * g : 128 * g + 128] = plus
                        left[1, at : at + 8, 128 * g : 128 * g + 128] = minus
    lower_row = jnp.concatenate([lower[0:1]] * 3, axis=1)
    for parity in range(2):
        value = left[parity]
        high, low = split(value)
        both = jnp.concatenate([high, low], axis=1)
        cols = slice(384 * parity, 384 * parity + 384)
        hi_table = table_hi[slot, :, cols]
        lo_table = table_lo[slot, :, cols]
        contract = ((1,), (0,))
        coef = wide_dot(both, jnp.concatenate([hi_table, hi_table], axis=0), contract)
        coef = coef + wide_dot(high, lo_table, contract)
        column = 2.0 * lax.broadcasted_iota(jnp.int32, (1, 384), 1).astype(F32) + float(parity)
        second = column >= 768.0 - lower_row
        scales = []
        for member in range(2):
            degree = column - 1.0 if member else lower_row + column
            kept = jnp.where(second, 1.0, 0.0) if member else jnp.where(second, 0.0, 1.0)
            ratio = degree * (degree + 1.0) / float(767 * 768)
            square = ratio * ratio
            scale = jnp.concatenate([kept / (1.0 + rate * square) for rate in rates], axis=0)
            scales += [scale, scale]
        damped = coef * jnp.concatenate(scales, axis=0)
        high, low = split(damped)
        both = jnp.concatenate([high, low], axis=1)
        contract = ((1,), (1,))
        given = wide_dot(both, jnp.concatenate([hi_table, hi_table], axis=1), contract)
        given = given + wide_dot(high, lo_table, contract)
        if parity == 0:
            final = last[slot, 0:1, :]
            extra = jnp.sum(value[96:192] * final, axis=1, keepdims=True)
            fade = jnp.concatenate([1.0 / (1.0 + rate) for rate in rates] * 2, axis=0)
            back[parity, 0:96, :] = given[0:96]
            back[parity, 96:192, :] = given[96:192] + (extra * fade) * final
        else:
            back[parity] = given
    for member in range(2):
        for r in range(2):
            for f in range(3):
                for g in range(3):
                    parts = []
                    for z in range(2):
                        at = (((member * 2 + r) * 2 + z) * 3 + f) * 8
                        plus = back[0, at : at + 8, 128 * g : 128 * g + 128]
                        minus = back[1, at : at + 8, 128 * g : 128 * g + 128]
                        if member:
                            plus, minus = jnp.where(odd_lower, minus, plus), jnp.where(odd_lower, plus, minus)
                        north, south = plus + minus, plus - minus
                        parts.append(jnp.where(first, north, pltpu.roll(south, 1, 0)))
                        parts.append(jnp.where(first, pltpu.roll(north, 7, 0), south))
                    for k, value in enumerate(block_swap(parts)):
                        flat[pl.ds(rows_at(member, r, 4 * g + k, f, slot), 8), :] = value


def step_kernel(
    points, weights, strength, pair_slot, field_hbm, increment_hbm, legendre_hbm, out_hbm,
    field, increment, source, waves, flat, sent, got, left, back, by_lat, by_wave, table_hi, table_lo, last,
    rows_0, rows_1, rows_2, rows_3, folds_0, folds_1, folds_2, folds_3, sums_0, sums_1, sums_2, sums_3,
    steps_0, steps_1, steps_2, steps_3, tables_0, tables_1, tables_2, tables_3,
    load_sems, sems, store_sem,
):
    rows = (rows_0, rows_1, rows_2, rows_3)
    folds = (folds_0, folds_1, folds_2, folds_3)
    sums = (sums_0, sums_1, sums_2, sums_3)
    steps = (steps_0, steps_1, steps_2, steps_3)
    tables = (tables_0, tables_1, tables_2, tables_3)
    band, lev = lax.axis_index("band"), lax.axis_index("lev")
    me = band * 4 + lev
    here = lev * 32 + band
    light, heavy = band < LIGHT, band >= LIGHT
    loads = [
        pltpu.make_async_copy(field_hbm, field, load_sems.at[0]),
        pltpu.make_async_copy(increment_hbm, increment, load_sems.at[1]),
        pltpu.make_async_copy(legendre_hbm, source, load_sems.at[2]),
    ]
    for load in loads:
        load.start()
    for slot in range(3):
        for z in range(4):
            got[0, ALL * slot + LOWER : ALL * slot + ALL, 32 * z : 32 * z + LIGHT, :] = jnp.zeros(
                (ALL - LOWER, LIGHT, 128), F32
            )

    @pl.when(light)
    def _():
        for slot in range(3):
            got[1, ALL * slot + LOWER : ALL * slot + ALL, :, :] = jnp.zeros((ALL - LOWER, 128, 128), F32)

    barrier = pltpu.get_barrier_semaphore()
    greet_all(barrier, me)
    for slot, value in enumerate(wave_orders(pair_slot[...])):
        waves[slot] = value
    loads[0].wait()
    loads[1].wait()

    def every(work):
        def some(k, carry):
            for side in range(SIDES):
                pair = SIDES * k + side
                work(k, side, pair, points[pair].astype(F32))
            return carry

        lax.fori_loop(0, 12 // SIDES, some, 0)

    def fold(k, side, pair, count):
        fold_pair(field, increment, pair, count, rows[side], folds[side], k)
        sums[side][k] = jnp.zeros((2, 144, 128), F32)

    every(fold)

    def outward(slot, carry):
        def transform(k, side, pair, count):
            weight = weights[band * 12 + pair]
            forward_pair(slot, k, folds[side], pair, count, weight, waves[slot], tables[side], steps[side], flat)

        every(transform)
        for c in range(ALL):
            chunk = ALL * slot + c
            sent[0, chunk] = flat[pl.ds(pl.multiple_of(128 * chunk, 128), 128), :].T

        @pl.when(slot == 0)
        def _():
            pl.semaphore_wait(barrier, 127)

        for kind, count in ((light, LOWER), (heavy, ALL)):

            @pl.when(kind)
            def _():
                def send(b, z):
                    post(sent.at[0], got.at[0], chunks_of(slot, count), b * 4 + z, here, sems.at[0, slot], (b, z))

                to_everyone(band, lev, send)

        for c in range(ALL):
            chunk = ALL * slot + c
            got[0, chunk, pl.ds(here, 1), :] = sent[0, chunk, pl.ds(me, 1), :]
        return carry

    lax.fori_loop(0, 3, outward, 0)
    loads[2].wait()

    def prepare(slot, carry):
        prepare_legendre(slot, source, by_lat, by_wave, table_hi, table_lo, last)
        return carry

    lax.fori_loop(0, 3, prepare, 0)
    rates = []
    for z in range(2):
        for f in range(3):
            index = lax.broadcasted_iota(jnp.int32, (8, 1), 0)
            rate = jnp.zeros((8, 1), F32)
            for l in range(4):
                for side in range(2):
                    rate = jnp.where(index == 2 * l + side, strength[f, 4 * (2 * z + side) + l], rate)
            rates.append(rate)
    slots = pair_slot[...].astype(F32)

    def owned(slot, carry):
        @pl.when(light)
        def _():
            drained(flat, (127 - HEAVY) * LOWER + HEAVY * ALL, sems.at[0, slot, 1])

        @pl.when(heavy)
        def _():
            drained(flat, (128 - HEAVY) * LOWER + (HEAVY - 1) * ALL, sems.at[0, slot, 1])

        for c in range(ALL):
            chunk = ALL * slot + c
            flat[pl.ds(pl.multiple_of(128 * chunk, 128), 128), :] = got[0, chunk].T
        mine = (3 * me + slot).astype(F32)
        index = lax.broadcasted_iota(jnp.int32, (1, 384), 1).astype(F32)
        lower = jnp.sum(jnp.where(slots == mine, index, 0.0), axis=1, keepdims=True)
        lower = jnp.broadcast_to(lower, (8, 128))
        legendre_slot(slot, lower, rates, flat, left, back, table_hi, table_lo, last)
        for c in range(ALL):
            chunk = ALL * slot + c
            sent[1, chunk] = flat[pl.ds(pl.multiple_of(128 * chunk, 128), 128), :].T

        def send(b, z):
            for kind, count in ((b < LIGHT, LOWER), (b >= LIGHT, ALL)):

                @pl.when(kind)
                def _():
                    post(sent.at[1], got.at[1], chunks_of(slot, count), z * 32 + b, me, sems.at[1, slot], (b, z))

        to_everyone(band, lev, send)
        for c in range(LOWER):
            chunk = ALL * slot + c
            got[1, chunk, pl.ds(me, 1), :] = sent[1, chunk, pl.ds(here, 1), :]

        @pl.when(heavy)
        def _():
            for c in range(LOWER, ALL):
                chunk = ALL * slot + c
                got[1, chunk, pl.ds(me, 1), :] = sent[1, chunk, pl.ds(here, 1), :]

        return carry

    lax.fori_loop(0, 3, owned, 0)

    def homeward(slot, carry):
        @pl.when(light)
        def _():
            drained(flat, 127 * LOWER, sems.at[1, slot, 1])

        @pl.when(heavy)
        def _():
            drained(flat, 127 * ALL, sems.at[1, slot, 1])

        for c in range(ALL):
            chunk = ALL * slot + c
            flat[pl.ds(pl.multiple_of(128 * chunk, 128), 128), :] = got[1, chunk].T

        def transform(k, side, pair, count):
            inverse_pair(slot, k, flat, pair, count, waves[slot], tables[side], steps[side], sums[side])

        every(transform)
        return carry

    lax.fori_loop(0, 3, homeward, 0)

    def unfold(k, side, pair, count):
        unfold_pair(k, pair, count, sums[side], rows[side], field)

    every(unfold)
    store = pltpu.make_async_copy(field, out_hbm, store_sem)
    store.start()

    def finish(slot, carry):
        @pl.when(light)
        def _():
            drained(flat, 127 * LOWER, sems.at[0, slot, 0])
            drained(flat, (127 - HEAVY) * LOWER + HEAVY * ALL, sems.at[1, slot, 0])

        @pl.when(heavy)
        def _():
            drained(flat, 127 * ALL, sems.at[0, slot, 0])
            drained(flat, (128 - HEAVY) * LOWER + (HEAVY - 1) * ALL, sems.at[1, slot, 0])

        return carry

    lax.fori_loop(0, 3, finish, 0)
    store.wait()


ANYWHERE = pl.BlockSpec(memory_space=pl.ANY)
SCALARS = pl.BlockSpec(memory_space=pltpu.SMEM)


def body(field_grid, increment, points, weights, pair_slot, legendre, strength):
    grid = (3, 4, 12, 2, 1536)
    each = 12 // SIDES
    return pl.pallas_call(
        step_kernel,
        out_shape=jax.ShapeDtypeStruct(grid, F32),
        in_specs=[SCALARS, SCALARS, SCALARS, pl.BlockSpec(memory_space=pltpu.VMEM), ANYWHERE, ANYWHERE, ANYWHERE],
        out_specs=ANYWHERE,
        scratch_shapes=[
            pltpu.VMEM(grid, F32),
            pltpu.VMEM(grid, F32),
            pltpu.VMEM((3, 769, 384), F32),
            pltpu.VMEM((3, 1, 256), F32),
            pltpu.VMEM((3456, 128), F32),
            pltpu.VMEM((2, 27, 128, 128), F32),
            pltpu.VMEM((2, 27, 128, 128), F32),
            pltpu.VMEM((2, 192, 384), F32),
            pltpu.VMEM((2, 192, 384), F32),
            pltpu.VMEM((3, 768, 128), F32),
            pltpu.VMEM((7, 384, 128), F32),
            pltpu.VMEM((3, 384, 768), BF16),
            pltpu.VMEM((3, 384, 768), BF16),
            pltpu.VMEM((3, 8, 384), F32),
        ]
        + [pltpu.VMEM((24, 1536), F32)] * SIDES
        + [pltpu.VMEM((each, 2, 144, 256), BF16)] * SIDES
        + [pltpu.VMEM((each, 2, 144, 128), F32)] * SIDES
        + [pltpu.VMEM((3, each, 2, 8, 256), F32)] * SIDES
        + [pltpu.VMEM((3, each, 4, 128, 256), BF16)] * SIDES
        + [
            pltpu.SemaphoreType.DMA((3,)),
            pltpu.SemaphoreType.DMA((2, 3, 2)),
            pltpu.SemaphoreType.DMA,
        ],
        compiler_params=pltpu.CompilerParams(
            collective_id=0, has_side_effects=True, vmem_limit_bytes=60 * 1024 * 1024
        ),
        name="spectral_step",
    )(points, weights, strength, pair_slot.reshape(1, 384), field_grid, increment, jnp.swapaxes(legendre, 1, 2))


def solution(mesh):
    return jax.shard_map(
        body,
        mesh=mesh,
        in_specs=(
            P(None, "lev", "band", None, None),
            P(None, "lev", "band", None, None),
            P("band"),
            P(),
            P(),
            P(("band", "lev"), None, None),
            P(),
        ),
        out_specs=P(None, "lev", "band", None, None),
        check_vma=False,
    )
```

```python
import math

import jax
import jax.numpy as jnp
from jax import lax
from jax.experimental import pallas as pl
from jax.experimental.pallas import tpu as pltpu
from jax.sharding import PartitionSpec as P

MESH = pl.DeviceIdType.MESH
F32 = jnp.float32
BF16 = jnp.bfloat16
SIN_COEFS = [(-1) ** k * math.pi ** (2 * k + 1) / math.factorial(2 * k + 1) for k in range(7)]
COS_COEFS = [(-1) ** k * math.pi ** (2 * k) / math.factorial(2 * k) for k in range(8)]


def half_turn_pair(half):
    square = half * half
    sine = jnp.full_like(square, SIN_COEFS[-1])
    for coef in SIN_COEFS[-2::-1]:
        sine = sine * square + coef
    cosine = jnp.full_like(square, COS_COEFS[-1])
    for coef in COS_COEFS[-2::-1]:
        cosine = cosine * square + coef
    return cosine, sine * half


def turn_pair(orders, doubled, count):
    period = 2.0 * count
    product = orders * doubled
    rest = product - jnp.round(product / period) * period
    cosine, sine = half_turn_pair(rest / period)
    return 1.0 - 2.0 * sine * sine, 2.0 * sine * cosine


def split(value):
    high = value.astype(BF16)
    return high, (value - high.astype(F32)).astype(BF16)


def wide_dot(left, right, contract):
    return lax.dot_general(left, right, (contract, ((), ())), preferred_element_type=F32)


def phase_rows(orders, count):
    row = lax.broadcasted_iota(jnp.int32, (8, orders.shape[1]), 0)
    fine = 2 * row + 1
    step = jnp.where(row < 4, jnp.left_shift(16, jnp.minimum(row, 4)), (row - 4) * 512 + 256)
    step = jnp.where(row == 7, 1535, step)
    wide = jnp.broadcast_to(orders, (8, orders.shape[1]))
    fine_pair = turn_pair(wide, fine.astype(F32), count)
    step_pair = turn_pair(wide, step.astype(F32), count)
    return fine_pair, step_pair


def fill_tables(fine_pair, step_pair, tables, index):
    cosine, sine = fine_pair
    step_cos, step_sin = step_pair
    for level in range(4):
        turn_cos = step_cos[level : level + 1]
        turn_sin = step_sin[level : level + 1]
        next_cos = cosine * turn_cos - sine * turn_sin
        next_sin = sine * turn_cos + cosine * turn_sin
        cosine = jnp.concatenate([cosine, next_cos], axis=0)
        sine = jnp.concatenate([sine, next_sin], axis=0)
    for n, value in enumerate((cosine, sine)):
        high, low = split(value)
        tables[(*index, 2 * n)] = high
        tables[(*index, 2 * n + 1)] = low


def reversed_lanes(value):
    index = 127 - lax.broadcasted_iota(jnp.int32, value.shape, 1)
    return jnp.take_along_axis(value, index, axis=1)


def block_swap(parts):
    lane = lax.broadcasted_iota(jnp.int32, parts[0].shape, 1)
    far = lane < 64
    near = (lane // 32) % 2 == 0
    a, b, c, d = parts
    a, c = jnp.where(far, a, pltpu.roll(c, 64, 1)), jnp.where(far, pltpu.roll(a, 64, 1), c)
    b, d = jnp.where(far, b, pltpu.roll(d, 64, 1)), jnp.where(far, pltpu.roll(b, 64, 1), d)
    a, b = jnp.where(near, a, pltpu.roll(b, 32, 1)), jnp.where(near, pltpu.roll(a, 96, 1), b)
    c, d = jnp.where(near, c, pltpu.roll(d, 32, 1)), jnp.where(near, pltpu.roll(c, 96, 1), d)
    return a, b, c, d


def greet_all(barrier, me):
    def greet(k, carry):
        t = lax.rem(me + k, 128)
        pl.semaphore_signal(barrier, inc=1, device_id=(t // 4, lax.rem(t, 4)), device_id_type=MESH)
        return carry

    lax.fori_loop(1, 128, greet, 0)


LIGHT = 15
ALL = 9
LOWER = 5
HEAVY = (32 - LIGHT) * 4
SIDES = 4


def chunks_of(slot, count):
    return pl.ds(ALL * slot, count)


def post(source, target, chunks, row, place, sems, device):
    pltpu.make_async_remote_copy(
        src_ref=source.at[chunks, pl.ds(row, 1), :],
        dst_ref=target.at[chunks, pl.ds(place, 1), :],
        send_sem=sems.at[0],
        recv_sem=sems.at[1],
        device_id=device,
        device_id_type=MESH,
    ).start()


def drained(ref, count, sem):
    pltpu.make_async_copy(ref.at[pl.ds(0, count), :], ref.at[pl.ds(0, count), :], sem).wait()


def to_everyone(band, lev, send):
    y, x, core = band // 8, (band // 2) % 4, band % 2
    cores = [core, 1 - core]
    levs = [lax.rem(lev + n, 4) for n in range(4)]

    def some(t, carry):
        ys = [lax.rem(y + lax.div(t, 4) + n, 4) for n in range(4)]
        xs = [lax.rem(x + lax.rem(t, 4) + n, 4) for n in range(4)]
        for n in range(8):
            b = ys[n % 4] * 8 + xs[n // 2] * 2 + cores[n // 4]
            z = levs[n % 4]
            if n == 0:

                @pl.when(t > 0)
                def _():
                    send(b, z)

            else:
                send(b, z)
        return carry

    lax.fori_loop(0, 16, some, 0)


def to_everyone_home(band, lev, send):
    y, x, core = band // 8, (band // 2) % 4, band % 2
    cores = [core, 1 - core]
    levs = [lax.rem(lev + n, 4) for n in range(4)]

    def some(t, carry):
        flip = lax.rem(y + t, 2)
        xs = [lax.rem(x + lax.div(t, 2) + n, 4) for n in range(4)]
        for n in range(8):
            z = levs[n % 4]
            side = flip if n % 2 == 0 else 1 - flip
            b = side * 8 + xs[(n // 2 + 2) % 4] * 2 + cores[n // 4]
            b_heavy = (3 - side) * 8 + xs[n // 2] * 2 + cores[n // 4]
            self_heavy = (b_heavy == band) & (z == lev)
            self_light = (b == band) & (z == lev)
            if n == 0:

                @pl.when(jnp.logical_not(self_heavy))
                def _():
                    send(b_heavy, z, ALL)

                @pl.when(jnp.logical_not(self_light | (b == LIGHT)))
                def _():
                    send(b, z, LOWER)

            else:
                send(b_heavy, z, ALL)

                @pl.when(b != LIGHT)
                def _():
                    send(b, z, LOWER)

        return carry

    lax.fori_loop(0, 8, some, 0)
    for z in levs:

        @pl.when(jnp.logical_not((band == LIGHT) & (z == lev)))
        def _():
            send(LIGHT, z, ALL)


def wave_orders(pair_slot):
    lanes = jnp.broadcast_to(pair_slot, (128, 384))
    column = jnp.concatenate([lanes[:, 128 * c : 128 * c + 128].T for c in range(3)], axis=0)
    wave = lax.broadcasted_iota(jnp.int32, (384, 128), 0).astype(F32)
    lane = lax.broadcasted_iota(jnp.int32, (384, 128), 1).astype(F32)
    lower = [jnp.sum(jnp.where(column == 3.0 * lane + s, wave, 0.0), axis=0, keepdims=True) for s in range(3)]
    return [jnp.concatenate([value, 767.0 - value], axis=1) for value in lower]


def rows_at(member, r, pair, f=0, slot=0):
    return pl.multiple_of(member * 576 + r * 24 + f * 8 + pair * 48 + slot * 1152, 8)


def fold_pair(field, increment, pair, count, rows, folds, index):
    for f in range(3):
        for l in range(4):
            at = 8 * f + 2 * l
            rows[at : at + 2, :] = field[f, l, pair] + increment[f, l, pair]
    value = rows[...]
    place = lax.broadcasted_iota(jnp.int32, value.shape, 1).astype(F32)
    value = jnp.where(place < count, value, 0.0)
    even, odd = [], []
    for block in range(6):
        low = reversed_lanes(value[:, 256 * block : 256 * block + 128])
        high = value[:, 256 * block + 128 : 256 * block + 256]
        even.append(high + low)
        odd.append(high - low)
    for n, parts in enumerate((even, odd)):
        whole = jnp.concatenate(
            [parts[3 + g] + parts[2 - g] for g in range(3)] + [parts[3 + g] - parts[2 - g] for g in range(3)],
            axis=0,
        )
        high, low = split(whole)
        folds[index, n, :, 0:128] = high
        folds[index, n, :, 128:256] = low


def forward_pair(slot, k, folds, pair, count, weight, orders, tables, steps, flat):
    fine_pair, step_pair = phase_rows(orders, count)
    fill_tables(fine_pair, step_pair, tables, (slot, k))
    step_cos, step_sin = step_pair
    steps[slot, k, 0] = step_cos
    steps[slot, k, 1] = step_sin

    def product(n):
        both = folds[k, n]
        table_hi, table_lo = tables[slot, k, 2 * n], tables[slot, k, 2 * n + 1]
        contract = ((1,), (0,))
        twice = jnp.concatenate([table_hi, table_hi], axis=0)
        return wide_dot(both, twice, contract) + wide_dot(both[:, 0:128], table_lo, contract)

    by_cos = product(0)
    by_sin = product(1)
    real = jnp.zeros((24, 256), F32)
    imag = jnp.zeros((24, 256), F32)
    for g in range(3):
        plus = slice(24 * g, 24 * g + 24)
        minus = slice(72 + 24 * g, 96 + 24 * g)
        turn_cos = step_cos[4 + g : 5 + g]
        turn_sin = step_sin[4 + g : 5 + g]
        real = real + turn_cos * by_cos[plus] - turn_sin * by_sin[minus]
        imag = imag - turn_sin * by_cos[minus] - turn_cos * by_sin[plus]
    live = (2.0 * orders + 1.0 <= count).astype(F32) * (weight / count)
    centre_cos = step_cos[7:8] * live
    centre_sin = step_sin[7:8] * live
    both = (real * centre_cos + imag * centre_sin, imag * centre_cos - real * centre_sin)
    for member in range(2):
        for r in range(2):
            flat[pl.ds(rows_at(member, r, pair, 0, slot), 24), :] = both[r][:, 128 * member : 128 * member + 128]


def inverse_pair(slot, k, flat, pair, count, orders, tables, steps, sums):
    step_cos, step_sin = steps[slot, k, 0], steps[slot, k, 1]

    def part(r):
        return jnp.concatenate(
            [flat[pl.ds(rows_at(member, r, pair, 0, slot), 24), :] for member in range(2)], axis=1
        )

    in_real, in_imag = part(0), part(1)
    live = 2.0 * orders + 1.0 <= count
    doubling = jnp.where(live, jnp.where(orders < 0.5, 1.0, 2.0), 0.0)
    centre_cos = step_cos[7:8] * doubling
    centre_sin = step_sin[7:8] * doubling
    real = in_real * centre_cos - in_imag * centre_sin
    imag = in_real * centre_sin + in_imag * centre_cos

    def turned(first, second):
        return jnp.concatenate(
            [first * step_cos[4 + g : 5 + g] for g in range(3)]
            + [second * step_sin[4 + g : 5 + g] for g in range(3)],
            axis=0,
        )

    def product(first, second, n):
        high, low = split(turned(first, second))
        contract = ((1,), (1,))
        table_hi, table_lo = tables[slot, k, 2 * n], tables[slot, k, 2 * n + 1]
        both = wide_dot(high, jnp.concatenate([table_hi, table_lo], axis=0), contract)
        return both[:, :128] + both[:, 128:] + wide_dot(low, table_hi, contract)

    by_cos = product(real, imag, 0)
    by_sin = product(imag, real, 1)
    sums[k, 0] = sums[k, 0] + by_cos
    sums[k, 1] = sums[k, 1] + by_sin


def unfold_pair(k, pair, count, sums, grid):
    by_cos, by_sin = sums[k, 0], sums[k, 1]
    place = lax.broadcasted_iota(jnp.int32, (24, 128), 1).astype(F32)

    def put(block, value):
        value = jnp.where(place + 128.0 * block < count, value, 0.0)
        for f in range(3):
            for l in range(4):
                at = 8 * f + 2 * l
                grid[f, l, pair, :, 128 * block : 128 * block + 128] = value[at : at + 2]

    for g in range(3):
        c1, c2 = by_cos[24 * g : 24 * g + 24], by_cos[72 + 24 * g : 96 + 24 * g]
        s1, s2 = by_sin[24 * g : 24 * g + 24], by_sin[72 + 24 * g : 96 + 24 * g]
        minus, plus = c1 - c2, c1 + c2
        total, differ = s1 + s2, s1 - s2
        put(2 * (3 + g) + 1, minus - total)
        put(2 * (3 + g), reversed_lanes(minus + total))
        put(2 * (2 - g) + 1, plus - differ)
        put(2 * (2 - g), reversed_lanes(plus + differ))


def pass_kernel(source, target, held, in_sems, out_sems):
    parts = [(f, l) for f in range(3) for l in range(4)]
    takes = [pltpu.make_async_copy(source.at[p], held.at[p], in_sems.at[n]) for n, p in enumerate(parts)]
    gives = [pltpu.make_async_copy(held.at[p], target.at[p], out_sems.at[n]) for n, p in enumerate(parts)]
    for take in takes:
        take.start()
    for take, give in zip(takes, gives):
        take.wait()
        give.start()
    for give in gives:
        give.wait()


def prepare_legendre(slot, source, by_lat, by_wave, table_hi, table_lo, last):
    for t in range(3):
        by_lat[t] = source[slot, 0:768, 128 * t : 128 * t + 128]
    for t in range(3):
        for parity in range(2):
            for c in range(3):
                chunk = by_lat[t, pl.ds(256 * c + parity, 128, stride=2), :]
                by_wave[3 * parity + c, 128 * t : 128 * t + 128, :] = chunk.T
        final = jnp.broadcast_to(source[slot, 768:769, 128 * t : 128 * t + 128], (128, 128))
        by_wave[6, 128 * t : 128 * t + 128, :] = final.T
    for i in range(12):
        for c in range(6):
            high, low = split(by_wave[c, pl.ds(i, 32, stride=12), :])
            table_hi[slot, 32 * i : 32 * i + 32, 128 * c : 128 * c + 128] = high
            table_lo[slot, 32 * i : 32 * i + 32, 128 * c : 128 * c + 128] = low
    for t in range(3):
        column = jnp.concatenate([by_wave[6, pl.ds(4 * t + k, 32, stride=12), :] for k in range(4)], axis=0)
        last[slot, :, 128 * t : 128 * t + 128] = column.T[0:8]


def legendre_slot(slot, lower, rates, flat, left, back, table_hi, table_lo, last):
    row = lax.broadcasted_iota(jnp.int32, (8, 128), 0)
    first = row % 2 == 0
    half_lower = lower * 0.5
    odd_lower = lower - 2.0 * jnp.floor(half_lower) > 0.5
    for member in range(2):
        for r in range(2):
            for f in range(3):
                for g in range(3):
                    parts = [flat[pl.ds(rows_at(member, r, 4 * g + k, f, slot), 8), :] for k in range(4)]
                    swapped = block_swap(parts)
                    for z in range(2):
                        a, b = swapped[2 * z], swapped[2 * z + 1]
                        north = jnp.where(first, a, pltpu.roll(b, 1, 0))
                        south = jnp.where(first, pltpu.roll(a, 7, 0), b)
                        plus, minus = north + south, north - south
                        if member:
                            plus, minus = jnp.where(odd_lower, minus, plus), jnp.where(odd_lower, plus, minus)
                        at = (((member * 2 + r) * 2 + z) * 3 + f) * 8
                        left[0, at : at + 8, 128 * g : 128 * g + 128] = plus
                        left[1, at : at + 8, 128 * g : 128 * g + 128] = minus
    lower_row = jnp.concatenate([lower[0:1]] * 3, axis=1)
    for parity in range(2):
        value = left[parity]
        high, low = split(value)
        both = jnp.concatenate([high, low], axis=1)
        cols = slice(384 * parity, 384 * parity + 384)
        hi_table = table_hi[slot, :, cols]
        lo_table = table_lo[slot, :, cols]
        contract = ((1,), (0,))
        coef = wide_dot(both, jnp.concatenate([hi_table, hi_table], axis=0), contract)
        coef = coef + wide_dot(high, lo_table, contract)
        column = 2.0 * lax.broadcasted_iota(jnp.int32, (1, 384), 1).astype(F32) + float(parity)
        second = column >= 768.0 - lower_row
        scales = []
        for member in range(2):
            degree = column - 1.0 if member else lower_row + column
            kept = jnp.where(second, 1.0, 0.0) if member else jnp.where(second, 0.0, 1.0)
            ratio = degree * (degree + 1.0) / float(767 * 768)
            square = ratio * ratio
            scale = jnp.concatenate([kept / (1.0 + rate * square) for rate in rates], axis=0)
            scales += [scale, scale]
        damped = coef * jnp.concatenate(scales, axis=0)
        high, low = split(damped)
        both = jnp.concatenate([high, low], axis=1)
        contract = ((1,), (1,))
        given = wide_dot(both, jnp.concatenate([hi_table, hi_table], axis=1), contract)
        given = given + wide_dot(high, lo_table, contract)
        if parity == 0:
            final = last[slot, 0:1, :]
            extra = jnp.sum(value[96:192] * final, axis=1, keepdims=True)
            fade = jnp.concatenate([1.0 / (1.0 + rate) for rate in rates] * 2, axis=0)
            back[parity, 0:96, :] = given[0:96]
            back[parity, 96:192, :] = given[96:192] + (extra * fade) * final
        else:
            back[parity] = given
    for member in range(2):
        for r in range(2):
            for f in range(3):
                for g in range(3):
                    parts = []
                    for z in range(2):
                        at = (((member * 2 + r) * 2 + z) * 3 + f) * 8
                        plus = back[0, at : at + 8, 128 * g : 128 * g + 128]
                        minus = back[1, at : at + 8, 128 * g : 128 * g + 128]
                        if member:
                            plus, minus = jnp.where(odd_lower, minus, plus), jnp.where(odd_lower, plus, minus)
                        north, south = plus + minus, plus - minus
                        parts.append(jnp.where(first, north, pltpu.roll(south, 1, 0)))
                        parts.append(jnp.where(first, pltpu.roll(north, 7, 0), south))
                    for k, value in enumerate(block_swap(parts)):
                        flat[pl.ds(rows_at(member, r, 4 * g + k, f, slot), 8), :] = value


def step_kernel(
    points, weights, strength, pair_slot, field_hbm, increment_hbm, legendre_hbm, out_hbm,
    field, increment, source, waves, flat, sent, got, left, back, by_lat, by_wave, table_hi, table_lo, last,
    grid, rows_0, rows_1, rows_2, rows_3, folds_0, folds_1, folds_2, folds_3, sums_0, sums_1, sums_2, sums_3,
    steps_0, steps_1, steps_2, steps_3, tables_0, tables_1, tables_2, tables_3,
    load_sems, legendre_sem, sems, store_sem,
):
    rows = (rows_0, rows_1, rows_2, rows_3)
    folds = (folds_0, folds_1, folds_2, folds_3)
    sums = (sums_0, sums_1, sums_2, sums_3)
    steps = (steps_0, steps_1, steps_2, steps_3)
    tables = (tables_0, tables_1, tables_2, tables_3)
    band, lev = lax.axis_index("band"), lax.axis_index("lev")
    me = band * 4 + lev
    here = lev * 32 + band
    light, heavy = band < LIGHT, band >= LIGHT
    loads = []
    for k in range(12 // SIDES):
        part = pl.ds(SIDES * k, SIDES)
        for n, (far, near) in enumerate(((field_hbm, field), (increment_hbm, increment))):
            loads.append(pltpu.make_async_copy(far.at[:, :, part], near.at[:, :, part], load_sems.at[n, k]))
    load_legendre = pltpu.make_async_copy(legendre_hbm, source, legendre_sem)
    for load in loads:
        load.start()
    load_legendre.start()
    for slot in range(3):
        for z in range(4):
            got[0, ALL * slot + LOWER : ALL * slot + ALL, 32 * z : 32 * z + LIGHT, :] = jnp.zeros(
                (ALL - LOWER, LIGHT, 128), F32
            )

    @pl.when(light)
    def _():
        for slot in range(3):
            got[1, ALL * slot + LOWER : ALL * slot + ALL, :, :] = jnp.zeros((ALL - LOWER, 128, 128), F32)

    barrier = pltpu.get_barrier_semaphore()
    greet_all(barrier, me)
    slots = pair_slot[...].reshape(1, 384).astype(F32)
    for slot, value in enumerate(wave_orders(slots)):
        waves[slot] = value
    def every(work):
        def some(k, carry):
            for side in range(SIDES):
                pair = SIDES * k + side
                work(k, side, pair, points[pair].astype(F32))
            return carry

        lax.fori_loop(0, 12 // SIDES, some, 0)

    def fold(k, side, pair, count):
        fold_pair(field, increment, pair, count, rows[side], folds[side], k)
        sums[side][k] = jnp.zeros((2, 144, 128), F32)

    for k in range(12 // SIDES):
        loads[2 * k].wait()
        loads[2 * k + 1].wait()
        for side in range(SIDES):
            pair = SIDES * k + side
            fold(k, side, pair, points[pair].astype(F32))


    def outward(slot, carry):
        def transform(k, side, pair, count):
            weight = weights[band * 12 + pair]
            forward_pair(slot, k, folds[side], pair, count, weight, waves[slot], tables[side], steps[side], flat)

        every(transform)
        for c in range(ALL):
            chunk = ALL * slot + c
            sent[0, chunk] = flat[pl.ds(pl.multiple_of(128 * chunk, 128), 128), :].T

        @pl.when(slot == 0)
        def _():
            pl.semaphore_wait(barrier, 127)

        for kind, count in ((light, LOWER), (heavy, ALL)):

            @pl.when(kind)
            def _():
                def send(b, z):
                    post(sent.at[0], got.at[0], chunks_of(slot, count), b * 4 + z, here, sems.at[0, slot], (b, z))

                to_everyone(band, lev, send)

        for c in range(ALL):
            chunk = ALL * slot + c
            got[0, chunk, pl.ds(here, 1), :] = sent[0, chunk, pl.ds(me, 1), :]
        return carry

    lax.fori_loop(0, 3, outward, 0)
    load_legendre.wait()

    def prepare(slot, carry):
        prepare_legendre(slot, source, by_lat, by_wave, table_hi, table_lo, last)
        return carry

    lax.fori_loop(0, 3, prepare, 0)
    rates = []
    for z in range(2):
        for f in range(3):
            index = lax.broadcasted_iota(jnp.int32, (8, 1), 0)
            rate = jnp.zeros((8, 1), F32)
            for l in range(4):
                for side in range(2):
                    rate = jnp.where(index == 2 * l + side, strength[f, 4 * (2 * z + side) + l], rate)
            rates.append(rate)

    def owned(slot, carry):
        @pl.when(light)
        def _():
            drained(flat, (127 - HEAVY) * LOWER + HEAVY * ALL, sems.at[0, slot, 1])

        @pl.when(heavy)
        def _():
            drained(flat, (128 - HEAVY) * LOWER + (HEAVY - 1) * ALL, sems.at[0, slot, 1])

        for c in range(ALL):
            chunk = ALL * slot + c
            flat[pl.ds(pl.multiple_of(128 * chunk, 128), 128), :] = got[0, chunk].T
        mine = (3 * me + slot).astype(F32)
        index = lax.broadcasted_iota(jnp.int32, (1, 384), 1).astype(F32)
        lower = jnp.sum(jnp.where(slots == mine, index, 0.0), axis=1, keepdims=True)
        lower = jnp.broadcast_to(lower, (8, 128))
        legendre_slot(slot, lower, rates, flat, left, back, table_hi, table_lo, last)
        for c in range(ALL):
            chunk = ALL * slot + c
            sent[1, chunk] = flat[pl.ds(pl.multiple_of(128 * chunk, 128), 128), :].T

        def send(b, z, count):
            post(sent.at[1], got.at[1], chunks_of(slot, count), z * 32 + b, me, sems.at[1, slot], (b, z))

        to_everyone_home(band, lev, send)
        for c in range(LOWER):
            chunk = ALL * slot + c
            got[1, chunk, pl.ds(me, 1), :] = sent[1, chunk, pl.ds(here, 1), :]

        @pl.when(heavy)
        def _():
            for c in range(LOWER, ALL):
                chunk = ALL * slot + c
                got[1, chunk, pl.ds(me, 1), :] = sent[1, chunk, pl.ds(here, 1), :]

        return carry

    lax.fori_loop(0, 3, owned, 0)

    def homeward(slot, carry):
        @pl.when(light)
        def _():
            drained(flat, 127 * LOWER, sems.at[1, slot, 1])

        @pl.when(heavy)
        def _():
            drained(flat, 127 * ALL, sems.at[1, slot, 1])

        for c in range(ALL):
            chunk = ALL * slot + c
            flat[pl.ds(pl.multiple_of(128 * chunk, 128), 128), :] = got[1, chunk].T

        def some(k, carry):
            for side in range(SIDES):
                pair = SIDES * k + side
                count = points[pair].astype(F32)
                inverse_pair(slot, k, flat, pair, count, waves[slot], tables[side], steps[side], sums[side])

            @pl.when(slot == 2)
            def _():
                for side in range(SIDES):
                    pair = SIDES * k + side
                    unfold_pair(k, pair, points[pair].astype(F32), sums[side], grid)
                part = pl.ds(SIDES * k, SIDES)
                pltpu.make_async_copy(grid.at[:, :, part], out_hbm.at[:, :, part], store_sem).start()

            return carry

        lax.fori_loop(0, 12 // SIDES, some, 0)
        return carry

    lax.fori_loop(0, 3, homeward, 0)

    def finish(slot, carry):
        @pl.when(light)
        def _():
            drained(flat, 127 * LOWER, sems.at[0, slot, 0])
            drained(flat, (127 - HEAVY) * LOWER + HEAVY * ALL, sems.at[1, slot, 0])

        @pl.when(heavy)
        def _():
            drained(flat, 127 * ALL, sems.at[0, slot, 0])
            drained(flat, (128 - HEAVY) * LOWER + (HEAVY - 1) * ALL, sems.at[1, slot, 0])

        return carry

    lax.fori_loop(0, 3, finish, 0)
    pltpu.make_async_copy(grid, out_hbm, store_sem).wait()


ANYWHERE = pl.BlockSpec(memory_space=pl.ANY)
SCALARS = pl.BlockSpec(memory_space=pltpu.SMEM)


def body(field_grid, increment, points, weights, pair_slot, legendre, strength):
    grid = (3, 4, 12, 2, 1536)
    each = 12 // SIDES
    stepped = pl.pallas_call(
        step_kernel,
        out_shape=jax.ShapeDtypeStruct(grid, F32),
        in_specs=[SCALARS, SCALARS, SCALARS, pl.BlockSpec(memory_space=pltpu.VMEM), ANYWHERE, ANYWHERE, ANYWHERE],
        out_specs=ANYWHERE,
        scratch_shapes=[
            pltpu.VMEM(grid, F32),
            pltpu.VMEM(grid, F32),
            pltpu.VMEM((3, 769, 384), F32),
            pltpu.VMEM((3, 1, 256), F32),
            pltpu.VMEM((3456, 128), F32),
            pltpu.VMEM((2, 27, 128, 128), F32),
            pltpu.VMEM((2, 27, 128, 128), F32),
            pltpu.VMEM((2, 192, 384), F32),
            pltpu.VMEM((2, 192, 384), F32),
            pltpu.VMEM((3, 768, 128), F32),
            pltpu.VMEM((7, 384, 128), F32),
            pltpu.VMEM((3, 384, 768), BF16),
            pltpu.VMEM((3, 384, 768), BF16),
            pltpu.VMEM((3, 8, 384), F32),
            pltpu.VMEM(grid, F32),
        ]
        + [pltpu.VMEM((24, 1536), F32)] * SIDES
        + [pltpu.VMEM((each, 2, 144, 256), BF16)] * SIDES
        + [pltpu.VMEM((each, 2, 144, 128), F32)] * SIDES
        + [pltpu.VMEM((3, each, 2, 8, 256), F32)] * SIDES
        + [pltpu.VMEM((3, each, 4, 128, 256), BF16)] * SIDES
        + [
            pltpu.SemaphoreType.DMA((2, each)),
            pltpu.SemaphoreType.DMA,
            pltpu.SemaphoreType.DMA((2, 3, 2)),
            pltpu.SemaphoreType.DMA,
        ],
        compiler_params=pltpu.CompilerParams(
            collective_id=0, has_side_effects=True, vmem_limit_bytes=60 * 1024 * 1024
        ),
        name="spectral_step",
    )(points, weights, strength, pair_slot, field_grid, increment, jnp.swapaxes(legendre, 1, 2))
    return pl.pallas_call(
        pass_kernel,
        out_shape=jax.ShapeDtypeStruct(grid, F32),
        in_specs=[ANYWHERE],
        out_specs=ANYWHERE,
        scratch_shapes=[pltpu.VMEM(grid, F32), pltpu.SemaphoreType.DMA((12,)), pltpu.SemaphoreType.DMA((12,))],
        name="pass_on",
    )(stepped)


def solution(mesh):
    return jax.shard_map(
        body,
        mesh=mesh,
        in_specs=(
            P(None, "lev", "band", None, None),
            P(None, "lev", "band", None, None),
            P("band"),
            P(),
            P(),
            P(("band", "lev"), None, None),
            P(),
        ),
        out_specs=P(None, "lev", "band", None, None),
        check_vma=False,
    )
```

```python
import math

import jax
import jax.numpy as jnp
from jax import lax
from jax.experimental import pallas as pl
from jax.experimental.pallas import tpu as pltpu
from jax.sharding import PartitionSpec as P

MESH = pl.DeviceIdType.MESH
F32 = jnp.float32
BF16 = jnp.bfloat16
SIN_COEFS = [(-1) ** k * math.pi ** (2 * k + 1) / math.factorial(2 * k + 1) for k in range(7)]
COS_COEFS = [(-1) ** k * math.pi ** (2 * k) / math.factorial(2 * k) for k in range(8)]


def half_turn_pair(half):
    square = half * half
    sine = jnp.full_like(square, SIN_COEFS[-1])
    for coef in SIN_COEFS[-2::-1]:
        sine = sine * square + coef
    cosine = jnp.full_like(square, COS_COEFS[-1])
    for coef in COS_COEFS[-2::-1]:
        cosine = cosine * square + coef
    return cosine, sine * half


def turn_pair(orders, doubled, count):
    period = 2.0 * count
    product = orders * doubled
    rest = product - jnp.round(product / period) * period
    cosine, sine = half_turn_pair(rest / period)
    return 1.0 - 2.0 * sine * sine, 2.0 * sine * cosine


def split(value):
    high = value.astype(BF16)
    return high, (value - high.astype(F32)).astype(BF16)


def wide_dot(left, right, contract):
    return lax.dot_general(left, right, (contract, ((), ())), preferred_element_type=F32)


def phase_rows(orders, count):
    row = lax.broadcasted_iota(jnp.int32, (8, orders.shape[1]), 0)
    fine = 2 * row + 1
    step = jnp.where(row < 4, jnp.left_shift(16, jnp.minimum(row, 4)), (row - 4) * 512 + 256)
    step = jnp.where(row == 7, 1535, step)
    wide = jnp.broadcast_to(orders, (8, orders.shape[1]))
    fine_pair = turn_pair(wide, fine.astype(F32), count)
    step_pair = turn_pair(wide, step.astype(F32), count)
    return fine_pair, step_pair


def fill_tables(fine_pair, step_pair, tables, index):
    cosine, sine = fine_pair
    step_cos, step_sin = step_pair
    for level in range(4):
        turn_cos = step_cos[level : level + 1]
        turn_sin = step_sin[level : level + 1]
        next_cos = cosine * turn_cos - sine * turn_sin
        next_sin = sine * turn_cos + cosine * turn_sin
        cosine = jnp.concatenate([cosine, next_cos], axis=0)
        sine = jnp.concatenate([sine, next_sin], axis=0)
    for n, value in enumerate((cosine, sine)):
        high, low = split(value)
        tables[(*index, 2 * n)] = high
        tables[(*index, 2 * n + 1)] = low


def reversed_lanes(value):
    index = 127 - lax.broadcasted_iota(jnp.int32, value.shape, 1)
    return jnp.take_along_axis(value, index, axis=1)


def block_swap(parts):
    lane = lax.broadcasted_iota(jnp.int32, parts[0].shape, 1)
    far = lane < 64
    near = (lane // 32) % 2 == 0
    a, b, c, d = parts
    a, c = jnp.where(far, a, pltpu.roll(c, 64, 1)), jnp.where(far, pltpu.roll(a, 64, 1), c)
    b, d = jnp.where(far, b, pltpu.roll(d, 64, 1)), jnp.where(far, pltpu.roll(b, 64, 1), d)
    a, b = jnp.where(near, a, pltpu.roll(b, 32, 1)), jnp.where(near, pltpu.roll(a, 96, 1), b)
    c, d = jnp.where(near, c, pltpu.roll(d, 32, 1)), jnp.where(near, pltpu.roll(c, 96, 1), d)
    return a, b, c, d


def greet_all(barrier, me):
    def greet(k, carry):
        t = lax.rem(me + k, 128)
        pl.semaphore_signal(barrier, inc=1, device_id=(t // 4, lax.rem(t, 4)), device_id_type=MESH)
        return carry

    lax.fori_loop(1, 128, greet, 0)


LIGHT = 15
ALL = 9
LOWER = 5
HEAVY = (32 - LIGHT) * 4
SIDES = 4


def chunks_of(slot, count):
    return pl.ds(ALL * slot, count)


def post(source, target, chunks, row, place, sems, device):
    pltpu.make_async_remote_copy(
        src_ref=source.at[chunks, pl.ds(row, 1), :],
        dst_ref=target.at[chunks, pl.ds(place, 1), :],
        send_sem=sems.at[0],
        recv_sem=sems.at[1],
        device_id=device,
        device_id_type=MESH,
    ).start()


def drained(ref, count, sem):
    pltpu.make_async_copy(ref.at[pl.ds(0, count), :], ref.at[pl.ds(0, count), :], sem).wait()


def to_everyone(band, lev, send):
    y, x, core = band // 8, (band // 2) % 4, band % 2
    cores = [core, 1 - core]
    levs = [lax.rem(lev + n, 4) for n in range(4)]

    def some(t, carry):
        there = lax.rem(y + lax.div(t, 4), 4)
        xs = [lax.rem(x + lax.rem(t, 4) + n, 4) for n in range(4)]
        for n in range(8):
            b = there * 8 + xs[n // 2] * 2 + cores[n // 4]
            z = levs[n % 4]
            if n == 0:

                @pl.when(t > 0)
                def _():
                    send(b, z)

            else:
                send(b, z)
        return carry

    lax.fori_loop(0, 16, some, 0)


def to_everyone_home(band, lev, send):
    y, x, core = band // 8, (band // 2) % 4, band % 2
    cores = [core, 1 - core]
    levs = [lax.rem(lev + n, 4) for n in range(4)]

    def some(t, carry):
        flip = lax.rem(y + t, 2)
        xs = [lax.rem(x + lax.div(t, 2) + n, 4) for n in range(4)]
        for n in range(8):
            z = levs[n % 4]
            side = flip if n % 2 == 0 else 1 - flip
            b = side * 8 + xs[(n // 2 + 2) % 4] * 2 + cores[n // 4]
            b_heavy = (3 - side) * 8 + xs[n // 2] * 2 + cores[n // 4]
            self_heavy = (b_heavy == band) & (z == lev)
            self_light = (b == band) & (z == lev)
            if n == 0:

                @pl.when(jnp.logical_not(self_heavy))
                def _():
                    send(b_heavy, z, ALL)

                @pl.when(jnp.logical_not(self_light | (b == LIGHT)))
                def _():
                    send(b, z, LOWER)

            else:
                send(b_heavy, z, ALL)

                @pl.when(b != LIGHT)
                def _():
                    send(b, z, LOWER)

        return carry

    lax.fori_loop(0, 8, some, 0)
    for z in levs:

        @pl.when(jnp.logical_not((band == LIGHT) & (z == lev)))
        def _():
            send(LIGHT, z, ALL)


def wave_orders(pair_slot):
    lanes = jnp.broadcast_to(pair_slot, (128, 384))
    column = jnp.concatenate([lanes[:, 128 * c : 128 * c + 128].T for c in range(3)], axis=0)
    wave = lax.broadcasted_iota(jnp.int32, (384, 128), 0).astype(F32)
    lane = lax.broadcasted_iota(jnp.int32, (384, 128), 1).astype(F32)
    lower = [jnp.sum(jnp.where(column == 3.0 * lane + s, wave, 0.0), axis=0, keepdims=True) for s in range(3)]
    return [jnp.concatenate([value, 767.0 - value], axis=1) for value in lower]


def rows_at(member, r, pair, f=0, slot=0):
    return pl.multiple_of(member * 576 + r * 24 + f * 8 + pair * 48 + slot * 1152, 8)


def fold_pair(field, increment, pair, count, rows, folds, index):
    for f in range(3):
        for l in range(4):
            at = 8 * f + 2 * l
            rows[at : at + 2, :] = field[f, l, pair] + increment[f, l, pair]
    value = rows[...]
    place = lax.broadcasted_iota(jnp.int32, value.shape, 1).astype(F32)
    value = jnp.where(place < count, value, 0.0)
    even, odd = [], []
    for block in range(6):
        low = reversed_lanes(value[:, 256 * block : 256 * block + 128])
        high = value[:, 256 * block + 128 : 256 * block + 256]
        even.append(high + low)
        odd.append(high - low)
    for n, parts in enumerate((even, odd)):
        whole = jnp.concatenate(
            [parts[3 + g] + parts[2 - g] for g in range(3)] + [parts[3 + g] - parts[2 - g] for g in range(3)],
            axis=0,
        )
        high, low = split(whole)
        folds[index, n, :, 0:128] = high
        folds[index, n, :, 128:256] = low


def forward_pair(slot, k, folds, pair, count, weight, orders, tables, steps, flat):
    fine_pair, step_pair = phase_rows(orders, count)
    fill_tables(fine_pair, step_pair, tables, (slot, k))
    step_cos, step_sin = step_pair
    steps[slot, k, 0] = step_cos
    steps[slot, k, 1] = step_sin

    def product(n):
        both = folds[k, n]
        table_hi, table_lo = tables[slot, k, 2 * n], tables[slot, k, 2 * n + 1]
        contract = ((1,), (0,))
        twice = jnp.concatenate([table_hi, table_hi], axis=0)
        return wide_dot(both, twice, contract) + wide_dot(both[:, 0:128], table_lo, contract)

    by_cos = product(0)
    by_sin = product(1)
    real = jnp.zeros((24, 256), F32)
    imag = jnp.zeros((24, 256), F32)
    for g in range(3):
        plus = slice(24 * g, 24 * g + 24)
        minus = slice(72 + 24 * g, 96 + 24 * g)
        turn_cos = step_cos[4 + g : 5 + g]
        turn_sin = step_sin[4 + g : 5 + g]
        real = real + turn_cos * by_cos[plus] - turn_sin * by_sin[minus]
        imag = imag - turn_sin * by_cos[minus] - turn_cos * by_sin[plus]
    live = (2.0 * orders + 1.0 <= count).astype(F32) * (weight / count)
    centre_cos = step_cos[7:8] * live
    centre_sin = step_sin[7:8] * live
    both = (real * centre_cos + imag * centre_sin, imag * centre_cos - real * centre_sin)
    for member in range(2):
        for r in range(2):
            flat[pl.ds(rows_at(member, r, pair, 0, slot), 24), :] = both[r][:, 128 * member : 128 * member + 128]


def inverse_pair(slot, k, flat, pair, count, orders, tables, steps, sums):
    step_cos, step_sin = steps[slot, k, 0], steps[slot, k, 1]

    def part(r):
        return jnp.concatenate(
            [flat[pl.ds(rows_at(member, r, pair, 0, slot), 24), :] for member in range(2)], axis=1
        )

    in_real, in_imag = part(0), part(1)
    live = 2.0 * orders + 1.0 <= count
    doubling = jnp.where(live, jnp.where(orders < 0.5, 1.0, 2.0), 0.0)
    centre_cos = step_cos[7:8] * doubling
    centre_sin = step_sin[7:8] * doubling
    real = in_real * centre_cos - in_imag * centre_sin
    imag = in_real * centre_sin + in_imag * centre_cos

    def turned(first, second):
        return jnp.concatenate(
            [first * step_cos[4 + g : 5 + g] for g in range(3)]
            + [second * step_sin[4 + g : 5 + g] for g in range(3)],
            axis=0,
        )

    def product(first, second, n):
        high, low = split(turned(first, second))
        contract = ((1,), (1,))
        table_hi, table_lo = tables[slot, k, 2 * n], tables[slot, k, 2 * n + 1]
        both = wide_dot(high, jnp.concatenate([table_hi, table_lo], axis=0), contract)
        return both[:, :128] + both[:, 128:] + wide_dot(low, table_hi, contract)

    by_cos = product(real, imag, 0)
    by_sin = product(imag, real, 1)
    sums[k, 0] = sums[k, 0] + by_cos
    sums[k, 1] = sums[k, 1] + by_sin


def unfold_pair(k, pair, count, sums, grid):
    by_cos, by_sin = sums[k, 0], sums[k, 1]
    place = lax.broadcasted_iota(jnp.int32, (24, 128), 1).astype(F32)

    def put(block, value):
        value = jnp.where(place + 128.0 * block < count, value, 0.0)
        for f in range(3):
            for l in range(4):
                at = 8 * f + 2 * l
                grid[f, l, pair, :, 128 * block : 128 * block + 128] = value[at : at + 2]

    for g in range(3):
        c1, c2 = by_cos[24 * g : 24 * g + 24], by_cos[72 + 24 * g : 96 + 24 * g]
        s1, s2 = by_sin[24 * g : 24 * g + 24], by_sin[72 + 24 * g : 96 + 24 * g]
        minus, plus = c1 - c2, c1 + c2
        total, differ = s1 + s2, s1 - s2
        put(2 * (3 + g) + 1, minus - total)
        put(2 * (3 + g), reversed_lanes(minus + total))
        put(2 * (2 - g) + 1, plus - differ)
        put(2 * (2 - g), reversed_lanes(plus + differ))


def pass_kernel(source, target, held, in_sems, out_sems):
    parts = [(f, l) for f in range(3) for l in range(4)]
    takes = [pltpu.make_async_copy(source.at[p], held.at[p], in_sems.at[n]) for n, p in enumerate(parts)]
    gives = [pltpu.make_async_copy(held.at[p], target.at[p], out_sems.at[n]) for n, p in enumerate(parts)]
    for take in takes:
        take.start()
    for take, give in zip(takes, gives):
        take.wait()
        give.start()
    for give in gives:
        give.wait()


def prepare_legendre(slot, source, by_lat, by_wave, table_hi, table_lo, last):
    for t in range(3):
        by_lat[t] = source[slot, 0:768, 128 * t : 128 * t + 128]
    for t in range(3):
        for parity in range(2):
            for c in range(3):
                chunk = by_lat[t, pl.ds(256 * c + parity, 128, stride=2), :]
                by_wave[3 * parity + c, 128 * t : 128 * t + 128, :] = chunk.T
        final = jnp.broadcast_to(source[slot, 768:769, 128 * t : 128 * t + 128], (128, 128))
        by_wave[6, 128 * t : 128 * t + 128, :] = final.T
    for i in range(12):
        for c in range(6):
            high, low = split(by_wave[c, pl.ds(i, 32, stride=12), :])
            table_hi[slot, 32 * i : 32 * i + 32, 128 * c : 128 * c + 128] = high
            table_lo[slot, 32 * i : 32 * i + 32, 128 * c : 128 * c + 128] = low
    for t in range(3):
        column = jnp.concatenate([by_wave[6, pl.ds(4 * t + k, 32, stride=12), :] for k in range(4)], axis=0)
        last[slot, :, 128 * t : 128 * t + 128] = column.T[0:8]


def legendre_slot(slot, lower, rates, flat, left, back, table_hi, table_lo, last):
    row = lax.broadcasted_iota(jnp.int32, (8, 128), 0)
    first = row % 2 == 0
    half_lower = lower * 0.5
    odd_lower = lower - 2.0 * jnp.floor(half_lower) > 0.5
    for member in range(2):
        for r in range(2):
            for f in range(3):
                for g in range(3):
                    parts = [flat[pl.ds(rows_at(member, r, 4 * g + k, f, slot), 8), :] for k in range(4)]
                    swapped = block_swap(parts)
                    for z in range(2):
                        a, b = swapped[2 * z], swapped[2 * z + 1]
                        north = jnp.where(first, a, pltpu.roll(b, 1, 0))
                        south = jnp.where(first, pltpu.roll(a, 7, 0), b)
                        plus, minus = north + south, north - south
                        if member:
                            plus, minus = jnp.where(odd_lower, minus, plus), jnp.where(odd_lower, plus, minus)
                        at = (((member * 2 + r) * 2 + z) * 3 + f) * 8
                        left[0, at : at + 8, 128 * g : 128 * g + 128] = plus
                        left[1, at : at + 8, 128 * g : 128 * g + 128] = minus
    lower_row = jnp.concatenate([lower[0:1]] * 3, axis=1)
    for parity in range(2):
        value = left[parity]
        high, low = split(value)
        both = jnp.concatenate([high, low], axis=1)
        cols = slice(384 * parity, 384 * parity + 384)
        hi_table = table_hi[slot, :, cols]
        lo_table = table_lo[slot, :, cols]
        contract = ((1,), (0,))
        coef = wide_dot(both, jnp.concatenate([hi_table, hi_table], axis=0), contract)
        coef = coef + wide_dot(high, lo_table, contract)
        column = 2.0 * lax.broadcasted_iota(jnp.int32, (1, 384), 1).astype(F32) + float(parity)
        second = column >= 768.0 - lower_row
        scales = []
        for member in range(2):
            degree = column - 1.0 if member else lower_row + column
            kept = jnp.where(second, 1.0, 0.0) if member else jnp.where(second, 0.0, 1.0)
            ratio = degree * (degree + 1.0) / float(767 * 768)
            square = ratio * ratio
            scale = jnp.concatenate([kept / (1.0 + rate * square) for rate in rates], axis=0)
            scales += [scale, scale]
        damped = coef * jnp.concatenate(scales, axis=0)
        high, low = split(damped)
        both = jnp.concatenate([high, low], axis=1)
        contract = ((1,), (1,))
        given = wide_dot(both, jnp.concatenate([hi_table, hi_table], axis=1), contract)
        given = given + wide_dot(high, lo_table, contract)
        if parity == 0:
            final = last[slot, 0:1, :]
            extra = jnp.sum(value[96:192] * final, axis=1, keepdims=True)
            fade = jnp.concatenate([1.0 / (1.0 + rate) for rate in rates] * 2, axis=0)
            back[parity, 0:96, :] = given[0:96]
            back[parity, 96:192, :] = given[96:192] + (extra * fade) * final
        else:
            back[parity] = given
    for member in range(2):
        for r in range(2):
            for f in range(3):
                for g in range(3):
                    parts = []
                    for z in range(2):
                        at = (((member * 2 + r) * 2 + z) * 3 + f) * 8
                        plus = back[0, at : at + 8, 128 * g : 128 * g + 128]
                        minus = back[1, at : at + 8, 128 * g : 128 * g + 128]
                        if member:
                            plus, minus = jnp.where(odd_lower, minus, plus), jnp.where(odd_lower, plus, minus)
                        north, south = plus + minus, plus - minus
                        parts.append(jnp.where(first, north, pltpu.roll(south, 1, 0)))
                        parts.append(jnp.where(first, pltpu.roll(north, 7, 0), south))
                    for k, value in enumerate(block_swap(parts)):
                        flat[pl.ds(rows_at(member, r, 4 * g + k, f, slot), 8), :] = value


def step_kernel(
    points, weights, strength, pair_slot, field_hbm, increment_hbm, legendre_hbm, out_hbm,
    field, increment, source, waves, flat, sent, got, left, back, by_lat, by_wave, table_hi, table_lo, last,
    grid, rows_0, rows_1, rows_2, rows_3, folds_0, folds_1, folds_2, folds_3, sums_0, sums_1, sums_2, sums_3,
    steps_0, steps_1, steps_2, steps_3, tables_0, tables_1, tables_2, tables_3,
    load_sems, legendre_sem, sems, store_sem,
):
    rows = (rows_0, rows_1, rows_2, rows_3)
    folds = (folds_0, folds_1, folds_2, folds_3)
    sums = (sums_0, sums_1, sums_2, sums_3)
    steps = (steps_0, steps_1, steps_2, steps_3)
    tables = (tables_0, tables_1, tables_2, tables_3)
    band, lev = lax.axis_index("band"), lax.axis_index("lev")
    me = band * 4 + lev
    here = lev * 32 + band
    light, heavy = band < LIGHT, band >= LIGHT
    loads = []
    for k in range(12 // SIDES):
        part = pl.ds(SIDES * k, SIDES)
        for n, (far, near) in enumerate(((field_hbm, field), (increment_hbm, increment))):
            loads.append(pltpu.make_async_copy(far.at[:, :, part], near.at[:, :, part], load_sems.at[n, k]))
    load_legendre = pltpu.make_async_copy(legendre_hbm, source, legendre_sem)
    for load in loads:
        load.start()
    load_legendre.start()
    for slot in range(3):
        for z in range(4):
            got[0, ALL * slot + LOWER : ALL * slot + ALL, 32 * z : 32 * z + LIGHT, :] = jnp.zeros(
                (ALL - LOWER, LIGHT, 128), F32
            )

    @pl.when(light)
    def _():
        for slot in range(3):
            got[1, ALL * slot + LOWER : ALL * slot + ALL, :, :] = jnp.zeros((ALL - LOWER, 128, 128), F32)

    barrier = pltpu.get_barrier_semaphore()
    greet_all(barrier, me)
    slots = pair_slot[...].reshape(1, 384).astype(F32)
    for slot, value in enumerate(wave_orders(slots)):
        waves[slot] = value
    def every(work):
        def some(k, carry):
            for side in range(SIDES):
                pair = SIDES * k + side
                work(k, side, pair, points[pair].astype(F32))
            return carry

        lax.fori_loop(0, 12 // SIDES, some, 0)

    def fold(k, side, pair, count):
        fold_pair(field, increment, pair, count, rows[side], folds[side], k)
        sums[side][k] = jnp.zeros((2, 144, 128), F32)

    for k in range(12 // SIDES):
        loads[2 * k].wait()
        loads[2 * k + 1].wait()
        for side in range(SIDES):
            pair = SIDES * k + side
            fold(k, side, pair, points[pair].astype(F32))


    def outward(slot, carry):
        def transform(k, side, pair, count):
            weight = weights[band * 12 + pair]
            forward_pair(slot, k, folds[side], pair, count, weight, waves[slot], tables[side], steps[side], flat)

        every(transform)
        for c in range(ALL):
            chunk = ALL * slot + c
            sent[0, chunk] = flat[pl.ds(pl.multiple_of(128 * chunk, 128), 128), :].T

        @pl.when(slot == 0)
        def _():
            pl.semaphore_wait(barrier, 127)

        for kind, count in ((light, LOWER), (heavy, ALL)):

            @pl.when(kind)
            def _():
                def send(b, z):
                    post(sent.at[0], got.at[0], chunks_of(slot, count), b * 4 + z, here, sems.at[0, slot], (b, z))

                to_everyone(band, lev, send)

        for c in range(ALL):
            chunk = ALL * slot + c
            got[0, chunk, pl.ds(here, 1), :] = sent[0, chunk, pl.ds(me, 1), :]
        return carry

    lax.fori_loop(0, 3, outward, 0)
    load_legendre.wait()

    def prepare(slot, carry):
        prepare_legendre(slot, source, by_lat, by_wave, table_hi, table_lo, last)
        return carry

    lax.fori_loop(0, 3, prepare, 0)
    rates = []
    for z in range(2):
        for f in range(3):
            index = lax.broadcasted_iota(jnp.int32, (8, 1), 0)
            rate = jnp.zeros((8, 1), F32)
            for l in range(4):
                for side in range(2):
                    rate = jnp.where(index == 2 * l + side, strength[f, 4 * (2 * z + side) + l], rate)
            rates.append(rate)

    def owned(slot, carry):
        @pl.when(light)
        def _():
            drained(flat, (127 - HEAVY) * LOWER + HEAVY * ALL, sems.at[0, slot, 1])

        @pl.when(heavy)
        def _():
            drained(flat, (128 - HEAVY) * LOWER + (HEAVY - 1) * ALL, sems.at[0, slot, 1])

        for c in range(ALL):
            chunk = ALL * slot + c
            flat[pl.ds(pl.multiple_of(128 * chunk, 128), 128), :] = got[0, chunk].T
        mine = (3 * me + slot).astype(F32)
        index = lax.broadcasted_iota(jnp.int32, (1, 384), 1).astype(F32)
        lower = jnp.sum(jnp.where(slots == mine, index, 0.0), axis=1, keepdims=True)
        lower = jnp.broadcast_to(lower, (8, 128))
        legendre_slot(slot, lower, rates, flat, left, back, table_hi, table_lo, last)
        for c in range(ALL):
            chunk = ALL * slot + c
            sent[1, chunk] = flat[pl.ds(pl.multiple_of(128 * chunk, 128), 128), :].T

        def send(b, z, count):
            post(sent.at[1], got.at[1], chunks_of(slot, count), z * 32 + b, me, sems.at[1, slot], (b, z))

        to_everyone_home(band, lev, send)
        for c in range(LOWER):
            chunk = ALL * slot + c
            got[1, chunk, pl.ds(me, 1), :] = sent[1, chunk, pl.ds(here, 1), :]

        @pl.when(heavy)
        def _():
            for c in range(LOWER, ALL):
                chunk = ALL * slot + c
                got[1, chunk, pl.ds(me, 1), :] = sent[1, chunk, pl.ds(here, 1), :]

        return carry

    lax.fori_loop(0, 3, owned, 0)

    def homeward(slot, carry):
        @pl.when(light)
        def _():
            drained(flat, 127 * LOWER, sems.at[1, slot, 1])

        @pl.when(heavy)
        def _():
            drained(flat, 127 * ALL, sems.at[1, slot, 1])

        for c in range(ALL):
            chunk = ALL * slot + c
            flat[pl.ds(pl.multiple_of(128 * chunk, 128), 128), :] = got[1, chunk].T

        def some(k, carry):
            for side in range(SIDES):
                pair = SIDES * k + side
                count = points[pair].astype(F32)
                inverse_pair(slot, k, flat, pair, count, waves[slot], tables[side], steps[side], sums[side])

            @pl.when(slot == 2)
            def _():
                for side in range(SIDES):
                    pair = SIDES * k + side
                    unfold_pair(k, pair, points[pair].astype(F32), sums[side], grid)
                part = pl.ds(SIDES * k, SIDES)
                pltpu.make_async_copy(grid.at[:, :, part], out_hbm.at[:, :, part], store_sem).start()

            return carry

        lax.fori_loop(0, 12 // SIDES, some, 0)
        return carry

    lax.fori_loop(0, 3, homeward, 0)

    def finish(slot, carry):
        @pl.when(light)
        def _():
            drained(flat, 127 * LOWER, sems.at[0, slot, 0])
            drained(flat, (127 - HEAVY) * LOWER + HEAVY * ALL, sems.at[1, slot, 0])

        @pl.when(heavy)
        def _():
            drained(flat, 127 * ALL, sems.at[0, slot, 0])
            drained(flat, (128 - HEAVY) * LOWER + (HEAVY - 1) * ALL, sems.at[1, slot, 0])

        return carry

    lax.fori_loop(0, 3, finish, 0)
    pltpu.make_async_copy(grid, out_hbm, store_sem).wait()


ANYWHERE = pl.BlockSpec(memory_space=pl.ANY)
SCALARS = pl.BlockSpec(memory_space=pltpu.SMEM)


def body(field_grid, increment, points, weights, pair_slot, legendre, strength):
    grid = (3, 4, 12, 2, 1536)
    each = 12 // SIDES
    stepped = pl.pallas_call(
        step_kernel,
        out_shape=jax.ShapeDtypeStruct(grid, F32),
        in_specs=[SCALARS, SCALARS, SCALARS, pl.BlockSpec(memory_space=pltpu.VMEM), ANYWHERE, ANYWHERE, ANYWHERE],
        out_specs=ANYWHERE,
        scratch_shapes=[
            pltpu.VMEM(grid, F32),
            pltpu.VMEM(grid, F32),
            pltpu.VMEM((3, 769, 384), F32),
            pltpu.VMEM((3, 1, 256), F32),
            pltpu.VMEM((3456, 128), F32),
            pltpu.VMEM((2, 27, 128, 128), F32),
            pltpu.VMEM((2, 27, 128, 128), F32),
            pltpu.VMEM((2, 192, 384), F32),
            pltpu.VMEM((2, 192, 384), F32),
            pltpu.VMEM((3, 768, 128), F32),
            pltpu.VMEM((7, 384, 128), F32),
            pltpu.VMEM((3, 384, 768), BF16),
            pltpu.VMEM((3, 384, 768), BF16),
            pltpu.VMEM((3, 8, 384), F32),
            pltpu.VMEM(grid, F32),
        ]
        + [pltpu.VMEM((24, 1536), F32)] * SIDES
        + [pltpu.VMEM((each, 2, 144, 256), BF16)] * SIDES
        + [pltpu.VMEM((each, 2, 144, 128), F32)] * SIDES
        + [pltpu.VMEM((3, each, 2, 8, 256), F32)] * SIDES
        + [pltpu.VMEM((3, each, 4, 128, 256), BF16)] * SIDES
        + [
            pltpu.SemaphoreType.DMA((2, each)),
            pltpu.SemaphoreType.DMA,
            pltpu.SemaphoreType.DMA((2, 3, 2)),
            pltpu.SemaphoreType.DMA,
        ],
        compiler_params=pltpu.CompilerParams(
            collective_id=0, has_side_effects=True, vmem_limit_bytes=60 * 1024 * 1024
        ),
        name="spectral_step",
    )(points, weights, strength, pair_slot, field_grid, increment, jnp.swapaxes(legendre, 1, 2))
    return pl.pallas_call(
        pass_kernel,
        out_shape=jax.ShapeDtypeStruct(grid, F32),
        in_specs=[ANYWHERE],
        out_specs=ANYWHERE,
        scratch_shapes=[pltpu.VMEM(grid, F32), pltpu.SemaphoreType.DMA((12,)), pltpu.SemaphoreType.DMA((12,))],
        name="pass_on",
    )(stepped)


def solution(mesh):
    return jax.shard_map(
        body,
        mesh=mesh,
        in_specs=(
            P(None, "lev", "band", None, None),
            P(None, "lev", "band", None, None),
            P("band"),
            P(),
            P(),
            P(("band", "lev"), None, None),
            P(),
        ),
        out_specs=P(None, "lev", "band", None, None),
        check_vma=False,
    )
```
